128 devices in a mesh: io: 16 (over z, y), cmp: 8 (over x, core).
Axes of the slice: x: 4, y: 4, z: 4, core: 2. Of those that a mesh axis runs over, the one named last changes fastest.
Arguments:
- fields: float32 [6, 8, 1024, 4096], P(None, None, 'cmp', 'io'), may hold values from -6 to 6
- mean_old: float32 [6, 8, 1024, 3072], P(None, 'cmp', 'io'), may hold values from -6 to 6
- land_mask: int32 [8, 1024, 4096], P('cmp', 'io'), may hold values from 0 to 1, as said below
Outputs:
- mean_new: float32 [6, 8, 1024, 3072], P(None, 'cmp', 'io')
- level_rms: float32 [6, 8], P(None, 'cmp')
The draws below stay inside these ranges and needn't reach their ends.
Inputs may be any that keep to these rules, and one draw needn't show every extreme that they name: `land_mask`: each row (level, latitude) has between 1 and 3072 ocean points, and some row has exactly 3072.
All inputs are finite; a program needn't handle non-finite values.
Results may differ from the reference program's by a relative error of at most 0.00002.
Values sent between devices are 32-bit elements; how exact they have to be, the bound alone decides.
A program may use at most 128 MiB of HBM per device.

```python
import jax
import jax.numpy as jnp
from jax import lax

FIELDS = 6
NI = 4096
L = 8
STEPS = 3
NJ = 1024
W = 3072


def draw_land_mask(key, part):
    key_scale, key_lev, key_row, key_perm = jax.random.split(jax.random.fold_in(key, 17), 4)
    row_index = jnp.arange(NJ, dtype=jnp.int32)
    base = W * (NJ + 3 * row_index) // (4 * NJ)
    factor = jax.random.randint(key_scale, (L, NJ), 80, 101)
    counts = jnp.maximum(base[None, :] * factor // 100, 1)
    pick_level = jax.random.randint(key_lev, (), 0, L)
    pick_row = jax.random.randint(key_row, (), 0, NJ)
    chosen = (jnp.arange(L, dtype=jnp.int32)[:, None] == pick_level) & (row_index[None, :] == pick_row)
    counts = jnp.where(chosen, W, counts)
    order = jnp.broadcast_to(jnp.arange(NI, dtype=jnp.int32), (L, NJ, NI))
    shuffled = jax.random.permutation(key_perm, order, axis=-1, independent=True)
    return (shuffled < counts[:, :, None]).astype(jnp.int32)


def shard_levels(own_key, shape, cuts, least, top_value):
    level = 1.0
    for dim, blocks in cuts:
        steps = jax.random.uniform(jax.random.fold_in(jax.random.fold_in(own_key, 6), dim), (blocks,), jnp.float32, least / len(cuts), top_value / len(cuts))
        level = level * jnp.repeat(jnp.exp(steps), shape[dim] // blocks).reshape((-1,) + (1,) * (len(shape) - 1 - dim))
    return level


def noise(stream_key, shape, spread, bound, cuts=(), kind=jnp.bfloat16):
    drawn = spread * jax.random.normal(stream_key, shape, jnp.float32)
    if cuts:
        drawn = drawn * shard_levels(stream_key, shape, cuts, -0.22, 0.18)
    return jnp.clip(drawn, -bound, bound).astype(kind)


def setup_inputs(seed: int = 0) -> dict:
    key_of = jax.random.split(jax.random.key(seed), 4)
    fields = noise(key_of[0], (FIELDS, L, NJ, NI), 1.0, 6.0, ((2, 8), (3, 16)), jnp.float32)
    mean_old = noise(key_of[1], (FIELDS, L, NJ, W), 1.0, 6.0, ((1, 8), (2, 16)), jnp.float32)
    land_mask = draw_land_mask(jax.random.fold_in(key_of[3], 71), 0)
    return dict(fields=fields, mean_old=mean_old, land_mask=land_mask)


def pack_one(values, target):
    width_out = 3 * values.shape[-1] // 4
    return jnp.zeros((values.shape[0], width_out), jnp.float32).at[:, target].set(values, mode='drop')

def pack_fields(fields, land_mask):
    nfield, nlev, nrow, ncol = fields.shape
    width_out = 3 * ncol // 4
    position = (jnp.cumsum(land_mask, axis=-1) - 1).astype(jnp.int32)
    target = jnp.where(land_mask == 1, position, width_out).astype(jnp.int32)
    flat = fields.reshape(nfield, nlev * nrow, ncol)
    packed = jax.vmap(pack_one, in_axes=(1, 0), out_axes=1)(flat, target.reshape(nlev * nrow, ncol))
    return packed.reshape(nfield, nlev, nrow, width_out)

def reference(fields, mean_old, land_mask):
    packed = pack_fields(fields, land_mask)
    counts = lax.optimization_barrier(jnp.sum(land_mask, axis=-1)).astype(jnp.int32)
    in_row = jnp.arange(mean_old.shape[-1], dtype=jnp.int32)[None, None, :] < counts[:, :, None]
    mean_new = jnp.where(in_row[None], (STEPS * mean_old + packed) / (STEPS + 1.0), jnp.float32(0.0))
    square_sum = lax.optimization_barrier(jnp.sum(mean_new * mean_new, axis=(2, 3)))
    ocean_total = lax.optimization_barrier(jnp.sum(counts, axis=1)).astype(jnp.float32)
    level_rms = jnp.sqrt(square_sum / ocean_total[None, :] + 1e-06)
    return (mean_new, level_rms)
```

```python
import jax
import jax.numpy as jnp
from jax import lax
from jax.experimental import pallas as pl
from jax.experimental.pallas import tpu as pltpu
from jax.sharding import PartitionSpec as P

STEPS = 3
MESH = pl.DeviceIdType.MESH

FIELDS = 6
LON = 16
ROWS = 64
COLS = 256
CHUNKS = 32
OUT_CHUNKS = 24
PIECES = 2
PIECE_ROWS = ROWS // PIECES
GROUPS = ROWS // 8
PIECE_GROUPS = PIECE_ROWS // 8
ORDER = [(dx, dy, dc) for dy in (0, 1) for dc in (0, 1) for dx in (1, 3, 2, 0)]


def lanes_of(array, index):
    return jnp.take_along_axis(array, index, axis=1, mode="promise_in_bounds")


def plan_group(g, mask, place, arrive, count):
    rows = pl.ds(pl.multiple_of(g * 8, 8), 8)
    chunk = [mask[rows, pl.ds(c * 128, 128)] for c in range(CHUNKS)]
    stacked = jnp.concatenate(chunk, axis=0).astype(jnp.float32).astype(jnp.bfloat16)
    source = lax.broadcasted_iota(jnp.int32, (128, 256), 0)
    target = lax.broadcasted_iota(jnp.int32, (128, 256), 1)
    upto = ((source <= target) | (target >= 128)).astype(jnp.float32).astype(jnp.bfloat16)
    sums = jnp.dot(stacked, upto, preferred_element_type=jnp.float32).astype(jnp.int32)
    lane = lax.broadcasted_iota(jnp.int32, (8, 128), 1)
    base = jnp.zeros((8, 128), jnp.int32)
    state = []
    for c in range(CHUNKS):
        upto_here = sums[c * 8 : c * 8 + 8, :128]
        number = sums[c * 8 : c * 8 + 8, 128:]
        rank = (lane - base) & 127
        at = jnp.zeros((8, 128), jnp.int32)
        for step in (64, 32, 16, 8, 4, 2, 1):
            seen = lanes_of(upto_here, at + (step - 1))
            at = jnp.where(seen <= rank, at + step, at)
        place[g, pl.ds(c * 8, 8), :] = at
        moved = c - ((base + rank) >> 7)
        state.append(jnp.where(rank < number, moved, 0))
        base = base + number
    count[g] = base
    arrived = [jnp.zeros((8, 128), jnp.int32) for _ in range(CHUNKS)]
    for s in range(5):
        bit = 1 << s
        new_state = []
        for c in range(CHUNKS):
            kept = jnp.where((state[c] & bit) != 0, 0, state[c])
            if c + bit < CHUNKS:
                comes = (state[c + bit] & bit) != 0
                arrived[c] = jnp.where(comes, arrived[c] | bit, arrived[c])
                kept = jnp.where(comes, state[c + bit], kept)
            new_state.append(kept)
        state = new_state
    for c in range(CHUNKS):
        arrive[g, pl.ds(c * 8, 8), :] = arrived[c]


def pack_group(f, g, landed, old, new, place, arrive, count):
    rows = pl.ds(pl.multiple_of(g * 8, 8), 8)
    value = []
    for c in range(CHUNKS):
        raw = landed[f, c // 2, rows, pl.ds((c % 2) * 128, 128)]
        value.append(lanes_of(raw, place[g, pl.ds(c * 8, 8), :]))
    moves = [arrive[g, pl.ds(c * 8, 8), :] for c in range(CHUNKS)]
    for s in range(5):
        bit = 1 << s
        for c in range(CHUNKS - bit):
            if s < 4 or c < OUT_CHUNKS:
                value[c] = jnp.where((moves[c] & bit) != 0, value[c + bit], value[c])
    lane = lax.broadcasted_iota(jnp.int32, (8, 128), 1)
    left = count[g] - lane
    squares = jnp.zeros((8, 128), jnp.float32)
    for c in range(OUT_CHUNKS):
        columns = pl.ds(c * 128, 128)
        mean = (STEPS * old[f, rows, columns] + value[c]) * jnp.float32(1.0 / (STEPS + 1.0))
        mean = jnp.where(left > c * 128, mean, jnp.float32(0.0))
        new[f, rows, columns] = mean
        squares = squares + mean * mean
    return squares


def kernel(
    fields, mean_old, land_mask, mean_new, rms,
    landed, mask, old, new, place, arrive, count, total, parts,
    send_sem, recv_sem, mask_sem, old_sem, new_sem, part_send, part_recv,
):
    io, b = lax.axis_index("io"), lax.axis_index("cmp")
    x, core = b // 2, b % 2
    keeps = (io // 2) == b

    def greet(s, carry):
        pl.semaphore_signal(barrier, inc=1, device_id=(s, io // 2), device_id_type=MESH)
        pl.semaphore_signal(barrier, inc=1, device_id=(s, b), device_id_type=MESH)
        return carry

    barrier = pltpu.get_barrier_semaphore()
    lax.fori_loop(0, LON, greet, 0)
    mask_copy = pltpu.make_async_copy(land_mask.at[0], mask, mask_sem)
    mask_copy.start()
    old_copy = pltpu.make_async_copy(mean_old.at[:, 0], old, old_sem)
    old_copy.start()
    pl.semaphore_wait(barrier, 2 * LON)

    peers = []
    for dx, dy, dc in ORDER:
        level = lax.rem(x + dx, 4) * 2 + lax.rem(core + dc, 2)
        band = x * 4 + core * 2 + dy
        peers.append((level, band, dy, (band == io) & (level == b)))

    def send_piece(i, carry):
        f, first = i // PIECES, lax.rem(i, PIECES) * PIECE_ROWS
        for level, band, half, here in peers:
            rows = pl.ds(pl.multiple_of(half * ROWS + first, 8), PIECE_ROWS)
            source = fields.at[f, level, rows, :]
            target = landed.at[f, io, pl.ds(pl.multiple_of(first, 8), PIECE_ROWS), :]

            @pl.when(jnp.logical_not(here))
            def _():
                pltpu.make_async_remote_copy(
                    src_ref=source,
                    dst_ref=target,
                    send_sem=send_sem.at[i],
                    recv_sem=recv_sem.at[i],
                    device_id=(band, level),
                    device_id_type=MESH,
                ).start()

            @pl.when(here)
            def _():
                pltpu.make_async_copy(source, target, recv_sem.at[i]).start()

        return carry

    lax.fori_loop(0, FIELDS * PIECES, send_piece, 0)

    mask_copy.wait()

    def plan(g, carry):
        plan_group(g, mask, place, arrive, count)
        return carry

    lax.fori_loop(0, GROUPS, plan, 0)
    total[...] = jnp.zeros_like(total)
    old_copy.wait()

    def pack_piece(i, carry):
        f, first = i // PIECES, lax.rem(i, PIECES) * PIECE_ROWS
        rows = pl.ds(pl.multiple_of(first, 8), PIECE_ROWS)
        piece = landed.at[f, :, rows, :]
        pltpu.make_async_copy(piece, piece, recv_sem.at[i]).wait()

        def pack(k, squares):
            g = lax.rem(i, PIECES) * PIECE_GROUPS + k
            return squares + pack_group(f, g, landed, old, new, place, arrive, count)

        total[f] += lax.fori_loop(0, PIECE_GROUPS, pack, jnp.zeros((8, 128), jnp.float32))
        pltpu.make_async_copy(new.at[f, rows, :], mean_new.at[f, 0, rows, :], new_sem.at[i]).start()
        return carry

    lax.fori_loop(0, FIELDS * PIECES, pack_piece, 0)

    ocean = count[0]
    for g in range(1, GROUPS):
        ocean = ocean + count[g]
    lines = [jnp.sum(total[f], axis=0, keepdims=True) for f in range(FIELDS)]
    lines.append(jnp.sum(ocean.astype(jnp.float32), axis=0, keepdims=True))
    lines.append(jnp.zeros((1, 128), jnp.float32))
    parts[io] = jnp.concatenate(lines, axis=0)

    def send_part(s, carry):
        to = lax.rem(io + s, LON)
        pltpu.make_async_remote_copy(
            src_ref=parts.at[io],
            dst_ref=parts.at[io],
            send_sem=part_send,
            recv_sem=part_recv,
            device_id=(to, b),
            device_id_type=MESH,
        ).start()
        return carry

    lax.fori_loop(1, LON, send_part, 0)

    def finish(i, carry):
        f, first = i // PIECES, lax.rem(i, PIECES) * PIECE_ROWS
        rows = pl.ds(pl.multiple_of(first, 8), PIECE_ROWS)
        pltpu.make_async_copy(new.at[f, rows, :], mean_new.at[f, 0, rows, :], new_sem.at[i]).wait()
        piece = landed.at[f, :, rows, :]

        @pl.when(jnp.logical_not(keeps))
        def _():
            pltpu.make_async_copy(piece, piece, send_sem.at[i]).wait()

        @pl.when(keeps)
        def _():
            most = landed.at[f, pl.ds(0, LON - 1), rows, :]
            pltpu.make_async_copy(most, most, send_sem.at[i]).wait()

        return carry

    lax.fori_loop(0, FIELDS * PIECES, finish, 0)
    others = parts.at[pl.ds(0, LON - 1)]
    pltpu.make_async_copy(others, others, part_send).wait()
    pltpu.make_async_copy(others, others, part_recv).wait()
    everything = parts[0]
    for s in range(1, LON):
        everything = everything + parts[s]
    square_sum = jnp.sum(everything[:FIELDS], axis=1, keepdims=True)
    ocean_total = everything[FIELDS : FIELDS + 1, :1]
    rms[...] = jnp.sqrt(square_sum / ocean_total + 1e-06)


def on_device(fields, mean_old, land_mask):
    pieces = FIELDS * PIECES
    return pl.pallas_call(
        kernel,
        out_shape=(
            jax.ShapeDtypeStruct(mean_old.shape, jnp.float32),
            jax.ShapeDtypeStruct((FIELDS, 1), jnp.float32),
        ),
        in_specs=[pl.BlockSpec(memory_space=pl.ANY)] * 3,
        out_specs=(pl.BlockSpec(memory_space=pl.ANY), pl.BlockSpec(memory_space=pltpu.VMEM)),
        scratch_shapes=[
            pltpu.VMEM((FIELDS, LON, ROWS, COLS), jnp.float32),
            pltpu.VMEM((ROWS, CHUNKS * 128), jnp.int32),
            pltpu.VMEM((FIELDS, ROWS, OUT_CHUNKS * 128), jnp.float32),
            pltpu.VMEM((FIELDS, ROWS, OUT_CHUNKS * 128), jnp.float32),
            pltpu.VMEM((GROUPS, CHUNKS * 8, 128), jnp.int32),
            pltpu.VMEM((GROUPS, CHUNKS * 8, 128), jnp.int32),
            pltpu.VMEM((GROUPS, 8, 128), jnp.int32),
            pltpu.VMEM((FIELDS, 8, 128), jnp.float32),
            pltpu.VMEM((LON, 8, 128), jnp.float32),
            pltpu.SemaphoreType.DMA((pieces,)),
            pltpu.SemaphoreType.DMA((pieces,)),
            pltpu.SemaphoreType.DMA,
            pltpu.SemaphoreType.DMA,
            pltpu.SemaphoreType.DMA((pieces,)),
            pltpu.SemaphoreType.DMA,
            pltpu.SemaphoreType.DMA,
        ],
        compiler_params=pltpu.CompilerParams(
            collective_id=0, has_side_effects=True, vmem_limit_bytes=56 * 1024 * 1024
        ),
    )(fields, mean_old, land_mask)


def solution(mesh):
    in_specs = (P(None, None, "cmp", "io"), P(None, "cmp", "io", None), P("cmp", "io", None))
    out_specs = (P(None, "cmp", "io", None), P(None, "cmp"))
    return jax.shard_map(
        on_device, mesh=mesh, in_specs=in_specs, out_specs=out_specs, check_vma=False
    )
```

```python
import jax
import jax.numpy as jnp
from jax import lax
from jax.experimental import pallas as pl
from jax.experimental.pallas import tpu as pltpu
from jax.sharding import PartitionSpec as P

STEPS = 3
MESH = pl.DeviceIdType.MESH

FIELDS = 6
LON = 16
ROWS = 64
COLS = 256
CHUNKS = 32
OUT_CHUNKS = 24
PIECES = 2
PIECE_ROWS = ROWS // PIECES
GROUPS = ROWS // 8
PIECE_GROUPS = PIECE_ROWS // 8
ORDER = [(dx, dy, dc) for dc in (0, 1) for dx in (1, 3, 2, 0) for dy in (0, 1)]


def lanes_of(array, index):
    return jnp.take_along_axis(array, index, axis=1, mode="promise_in_bounds")


def plan_group(g, mask, place, arrive, count):
    rows = pl.ds(pl.multiple_of(g * 8, 8), 8)
    chunk = [mask[rows, pl.ds(c * 128, 128)] for c in range(CHUNKS)]
    stacked = jnp.concatenate(chunk, axis=0).astype(jnp.float32).astype(jnp.bfloat16)
    source = lax.broadcasted_iota(jnp.int32, (128, 256), 0)
    target = lax.broadcasted_iota(jnp.int32, (128, 256), 1)
    upto = ((source <= target) | (target >= 128)).astype(jnp.float32).astype(jnp.bfloat16)
    sums = jnp.dot(stacked, upto, preferred_element_type=jnp.float32).astype(jnp.int32)
    lane = lax.broadcasted_iota(jnp.int32, (8, 128), 1)
    base = jnp.zeros((8, 128), jnp.int32)
    state = []
    for c in range(CHUNKS):
        upto_here = sums[c * 8 : c * 8 + 8, :128]
        number = sums[c * 8 : c * 8 + 8, 128:]
        rank = (lane - base) & 127
        at = jnp.zeros((8, 128), jnp.int32)
        for step in (64, 32, 16, 8, 4, 2, 1):
            seen = lanes_of(upto_here, at + (step - 1))
            at = jnp.where(seen <= rank, at + step, at)
        place[g, pl.ds(c * 8, 8), :] = at
        moved = c - ((base + rank) >> 7)
        state.append(jnp.where(rank < number, moved, 0))
        base = base + number
    count[g] = base
    arrived = [jnp.zeros((8, 128), jnp.int32) for _ in range(CHUNKS)]
    for s in range(5):
        bit = 1 << s
        new_state = []
        for c in range(CHUNKS):
            kept = jnp.where((state[c] & bit) != 0, 0, state[c])
            if c + bit < CHUNKS:
                comes = (state[c + bit] & bit) != 0
                arrived[c] = jnp.where(comes, arrived[c] | bit, arrived[c])
                kept = jnp.where(comes, state[c + bit], kept)
            new_state.append(kept)
        state = new_state
    for c in range(CHUNKS):
        arrive[g, pl.ds(c * 8, 8), :] = arrived[c]


def pack_group(f, g, landed, old, new, place, arrive, count):
    rows = pl.ds(pl.multiple_of(g * 8, 8), 8)
    value = []
    for c in range(CHUNKS):
        raw = landed[f, c // 2, rows, pl.ds((c % 2) * 128, 128)]
        value.append(lanes_of(raw, place[g, pl.ds(c * 8, 8), :]))
    moves = [arrive[g, pl.ds(c * 8, 8), :] for c in range(CHUNKS)]
    for s in range(5):
        bit = 1 << s
        for c in range(CHUNKS - bit):
            if s < 4 or c < OUT_CHUNKS:
                value[c] = jnp.where((moves[c] & bit) != 0, value[c + bit], value[c])
    lane = lax.broadcasted_iota(jnp.int32, (8, 128), 1)
    left = count[g] - lane
    squares = jnp.zeros((8, 128), jnp.float32)
    for c in range(OUT_CHUNKS):
        columns = pl.ds(c * 128, 128)
        mean = (STEPS * old[f, rows, columns] + value[c]) * jnp.float32(1.0 / (STEPS + 1.0))
        mean = jnp.where(left > c * 128, mean, jnp.float32(0.0))
        new[f, 0, rows, columns] = mean
        squares = squares + mean * mean
    return squares


def kernel(
    fields, mean_old, land_mask, new, rms,
    landed, mask, old, place, arrive, count, total, parts,
    send_sem, recv_sem, mask_sem, old_sem, part_send, part_recv,
):
    io, b = lax.axis_index("io"), lax.axis_index("cmp")
    x, core = b // 2, b % 2
    keeps = (io // 2) == b

    def greet(s, carry):
        pl.semaphore_signal(barrier, inc=1, device_id=(s, io // 2), device_id_type=MESH)
        pl.semaphore_signal(barrier, inc=1, device_id=(s, b), device_id_type=MESH)
        return carry

    barrier = pltpu.get_barrier_semaphore()
    lax.fori_loop(0, LON, greet, 0)
    mask_copy = pltpu.make_async_copy(land_mask.at[0], mask, mask_sem)
    mask_copy.start()
    old_copy = pltpu.make_async_copy(mean_old.at[:, 0], old, old_sem)
    old_copy.start()
    pl.semaphore_wait(barrier, 2 * LON)

    peers = []
    for dx, dy, dc in ORDER:
        level = lax.rem(x + dx, 4) * 2 + lax.rem(core + dc, 2)
        half = lax.rem(io + io // 4 + dy, 2)
        band = x * 4 + core * 2 + half
        peers.append((level, band, half, (band == io) & (level == b)))

    def send_piece(i, carry):
        f, first = i // PIECES, lax.rem(i, PIECES) * PIECE_ROWS
        for level, band, half, here in peers:
            rows = pl.ds(pl.multiple_of(half * ROWS + first, 8), PIECE_ROWS)
            source = fields.at[f, level, rows, :]
            target = landed.at[f, io, pl.ds(pl.multiple_of(first, 8), PIECE_ROWS), :]

            @pl.when(jnp.logical_not(here))
            def _():
                pltpu.make_async_remote_copy(
                    src_ref=source,
                    dst_ref=target,
                    send_sem=send_sem.at[i],
                    recv_sem=recv_sem.at[i],
                    device_id=(band, level),
                    device_id_type=MESH,
                ).start()

            @pl.when(here)
            def _():
                pltpu.make_async_copy(source, target, recv_sem.at[i]).start()

        return carry

    lax.fori_loop(0, FIELDS * PIECES, send_piece, 0)

    mask_copy.wait()

    def plan(g, carry):
        plan_group(g, mask, place, arrive, count)
        return carry

    lax.fori_loop(0, GROUPS, plan, 0)
    total[...] = jnp.zeros_like(total)
    old_copy.wait()

    def pack_piece(i, carry):
        f, first = i // PIECES, lax.rem(i, PIECES) * PIECE_ROWS
        rows = pl.ds(pl.multiple_of(first, 8), PIECE_ROWS)
        piece = landed.at[f, :, rows, :]
        pltpu.make_async_copy(piece, piece, recv_sem.at[i]).wait()

        def pack(k, squares):
            g = lax.rem(i, PIECES) * PIECE_GROUPS + k
            return squares + pack_group(f, g, landed, old, new, place, arrive, count)

        total[f] += lax.fori_loop(0, PIECE_GROUPS, pack, jnp.zeros((8, 128), jnp.float32))
        return carry

    lax.fori_loop(0, FIELDS * PIECES, pack_piece, 0)

    ocean = count[0]
    for g in range(1, GROUPS):
        ocean = ocean + count[g]
    lines = [jnp.sum(total[f], axis=0, keepdims=True) for f in range(FIELDS)]
    lines.append(jnp.sum(ocean.astype(jnp.float32), axis=0, keepdims=True))
    lines.append(jnp.zeros((1, 128), jnp.float32))
    parts[io] = jnp.concatenate(lines, axis=0)

    def send_part(s, carry):
        to = lax.rem(io + s, LON)
        pltpu.make_async_remote_copy(
            src_ref=parts.at[io],
            dst_ref=parts.at[io],
            send_sem=part_send,
            recv_sem=part_recv,
            device_id=(to, b),
            device_id_type=MESH,
        ).start()
        return carry

    lax.fori_loop(1, LON, send_part, 0)

    def finish(i, carry):
        f, first = i // PIECES, lax.rem(i, PIECES) * PIECE_ROWS
        rows = pl.ds(pl.multiple_of(first, 8), PIECE_ROWS)
        piece = landed.at[f, :, rows, :]

        @pl.when(jnp.logical_not(keeps))
        def _():
            pltpu.make_async_copy(piece, piece, send_sem.at[i]).wait()

        @pl.when(keeps)
        def _():
            most = landed.at[f, pl.ds(0, LON - 1), rows, :]
            pltpu.make_async_copy(most, most, send_sem.at[i]).wait()

        return carry

    lax.fori_loop(0, FIELDS * PIECES, finish, 0)
    others = parts.at[pl.ds(0, LON - 1)]
    pltpu.make_async_copy(others, others, part_send).wait()
    pltpu.make_async_copy(others, others, part_recv).wait()
    everything = parts[0]
    for s in range(1, LON):
        everything = everything + parts[s]
    lane = lax.broadcasted_iota(jnp.int32, (1, 128), 1)
    square_sum = jnp.zeros((1, 128), jnp.float32)
    for f in range(FIELDS):
        field_sum = jnp.sum(everything[f : f + 1], axis=1, keepdims=True)
        square_sum = jnp.where(lane == f, field_sum, square_sum)
    ocean_total = everything[FIELDS : FIELDS + 1]
    rms[...] = jnp.sqrt(square_sum / ocean_total + 1e-06)


def write(new, rms, mean_new, level_rms, sem):
    def piece(i):
        f, first = i // PIECES, lax.rem(i, PIECES) * PIECE_ROWS
        rows = pl.ds(pl.multiple_of(first, 8), PIECE_ROWS)
        return pltpu.make_async_copy(new.at[f, 0, rows, :], mean_new.at[f, 0, rows, :], sem.at[i])

    for i in range(FIELDS * PIECES):
        piece(i).start()
    level_rms[...] = rms[:, :FIELDS]
    for i in range(FIELDS * PIECES):
        piece(i).wait()


def on_device(fields, mean_old, land_mask):
    pieces = FIELDS * PIECES
    fields, mean_old, land_mask = (
        pltpu.with_memory_space_constraint(a, pltpu.HBM) for a in (fields, mean_old, land_mask)
    )
    new, rms = pl.pallas_call(
        kernel,
        out_shape=(
            pltpu.VMEM(mean_old.shape, jnp.float32),
            pltpu.VMEM((1, 128), jnp.float32),
        ),
        in_specs=[pl.BlockSpec(memory_space=pltpu.HBM)] * 3,
        out_specs=[pl.BlockSpec(memory_space=pltpu.VMEM)] * 2,
        scratch_shapes=[
            pltpu.VMEM((FIELDS, LON, ROWS, COLS), jnp.float32),
            pltpu.VMEM((ROWS, CHUNKS * 128), jnp.int32),
            pltpu.VMEM((FIELDS, ROWS, OUT_CHUNKS * 128), jnp.float32),
            pltpu.VMEM((GROUPS, CHUNKS * 8, 128), jnp.int32),
            pltpu.VMEM((GROUPS, CHUNKS * 8, 128), jnp.int32),
            pltpu.VMEM((GROUPS, 8, 128), jnp.int32),
            pltpu.VMEM((FIELDS, 8, 128), jnp.float32),
            pltpu.VMEM((LON, 8, 128), jnp.float32),
            pltpu.SemaphoreType.DMA((pieces,)),
            pltpu.SemaphoreType.DMA((pieces,)),
            pltpu.SemaphoreType.DMA,
            pltpu.SemaphoreType.DMA,
            pltpu.SemaphoreType.DMA,
            pltpu.SemaphoreType.DMA,
        ],
        compiler_params=pltpu.CompilerParams(
            collective_id=0, has_side_effects=True, vmem_limit_bytes=20 * 1024 * 1024
        ),
    )(fields, mean_old, land_mask)
    mean_new, level_rms = pl.pallas_call(
        write,
        out_shape=(
            jax.ShapeDtypeStruct(mean_old.shape, jnp.float32),
            jax.ShapeDtypeStruct((1, FIELDS), jnp.float32),
        ),
        in_specs=[pl.BlockSpec(memory_space=pltpu.VMEM)] * 2,
        out_specs=(pl.BlockSpec(memory_space=pltpu.HBM), pl.BlockSpec(memory_space=pltpu.VMEM)),
        scratch_shapes=[pltpu.SemaphoreType.DMA((pieces,))],
        compiler_params=pltpu.CompilerParams(vmem_limit_bytes=8 * 1024 * 1024),
    )(new, rms)
    return mean_new, level_rms.reshape(FIELDS, 1)


def solution(mesh):
    in_specs = (P(None, None, "cmp", "io"), P(None, "cmp", "io", None), P("cmp", "io", None))
    out_specs = (P(None, "cmp", "io", None), P(None, "cmp"))
    return jax.shard_map(
        on_device, mesh=mesh, in_specs=in_specs, out_specs=out_specs, check_vma=False
    )
```

```python
import jax
import jax.numpy as jnp
from jax import lax
from jax.experimental import pallas as pl
from jax.experimental.pallas import tpu as pltpu
from jax.sharding import PartitionSpec as P

STEPS = 3
MESH = pl.DeviceIdType.MESH

FIELDS = 6
LON = 16
ROWS = 64
COLS = 256
CHUNKS = 32
OUT_CHUNKS = 24
GROUPS = ROWS // 8
LAST = FIELDS - 1
MAIN_ROWS, LAST_ROWS = 16, 8
PER_FIELD = ROWS // MAIN_ROWS
LAST_PIECES = MAIN_ROWS // LAST_ROWS
ARRIVALS = LAST + PER_FIELD - 1 + LAST_PIECES
ORDER = [(dx, dy, dc) for dc in (0, 1) for dx in (1, 3, 2, 0) for dy in (0, 1)]


def lanes_of(array, index):
    return jnp.take_along_axis(array, index, axis=1, mode="promise_in_bounds")


def plan_group(g, mask, place, arrive, count):
    rows = pl.ds(pl.multiple_of(g * 8, 8), 8)
    chunk = [mask[rows, pl.ds(c * 128, 128)] for c in range(CHUNKS)]
    stacked = jnp.concatenate(chunk, axis=0).astype(jnp.float32).astype(jnp.bfloat16)
    source = lax.broadcasted_iota(jnp.int32, (128, 256), 0)
    target = lax.broadcasted_iota(jnp.int32, (128, 256), 1)
    upto = ((source <= target) | (target >= 128)).astype(jnp.float32).astype(jnp.bfloat16)
    sums = jnp.dot(stacked, upto, preferred_element_type=jnp.float32).astype(jnp.int32)
    lane = lax.broadcasted_iota(jnp.int32, (8, 128), 1)
    base = jnp.zeros((8, 128), jnp.int32)
    state = []
    for c in range(CHUNKS):
        upto_here = sums[c * 8 : c * 8 + 8, :128]
        number = sums[c * 8 : c * 8 + 8, 128:]
        rank = (lane - base) & 127
        at = jnp.zeros((8, 128), jnp.int32)
        for step in (64, 32, 16, 8, 4, 2, 1):
            seen = lanes_of(upto_here, at + (step - 1))
            at = jnp.where(seen <= rank, at + step, at)
        place[g, pl.ds(c * 8, 8), :] = at
        moved = c - ((base + rank) >> 7)
        state.append(jnp.where(rank < number, moved, 0))
        base = base + number
    count[g] = base
    arrived = [jnp.zeros((8, 128), jnp.int32) for _ in range(CHUNKS)]
    for s in range(5):
        bit = 1 << s
        new_state = []
        for c in range(CHUNKS):
            kept = jnp.where((state[c] & bit) != 0, 0, state[c])
            if c + bit < CHUNKS:
                comes = (state[c + bit] & bit) != 0
                arrived[c] = jnp.where(comes, arrived[c] | bit, arrived[c])
                kept = jnp.where(comes, state[c + bit], kept)
            new_state.append(kept)
        state = new_state
    for c in range(CHUNKS):
        arrive[g, pl.ds(c * 8, 8), :] = arrived[c]


def pack_group(f, g, landed, old, new, place, arrive, count):
    rows = pl.ds(pl.multiple_of(g * 8, 8), 8)
    value = []
    for c in range(CHUNKS):
        raw = landed[f, c // 2, rows, pl.ds((c % 2) * 128, 128)]
        value.append(lanes_of(raw, place[g, pl.ds(c * 8, 8), :]))
    moves = [arrive[g, pl.ds(c * 8, 8), :] for c in range(CHUNKS)]
    for s in range(5):
        bit = 1 << s
        for c in range(CHUNKS - bit):
            if s < 4 or c < OUT_CHUNKS:
                value[c] = jnp.where((moves[c] & bit) != 0, value[c + bit], value[c])
    lane = lax.broadcasted_iota(jnp.int32, (8, 128), 1)
    left = count[g] - lane
    squares = jnp.zeros((8, 128), jnp.float32)
    for c in range(OUT_CHUNKS):
        columns = pl.ds(c * 128, 128)
        mean = (STEPS * old[f, rows, columns] + value[c]) * jnp.float32(1.0 / (STEPS + 1.0))
        mean = jnp.where(left > c * 128, mean, jnp.float32(0.0))
        new[f, 0, rows, columns] = mean
        squares = squares + mean * mean
    return squares


def kernel(
    fields, mean_old, land_mask, new, sums,
    staged, landed, mask, old, place, arrive, count, total, parts,
    stage_sem, send_sem, recv_sem, mask_sem, old_sem, part_send, part_recv,
):
    io, b = lax.axis_index("io"), lax.axis_index("cmp")
    x, core = b // 2, b % 2
    keeps = (io // 2) == b

    barrier = pltpu.get_barrier_semaphore()
    for s in range(LON):
        pl.semaphore_signal(barrier, inc=1, device_id=(s, io // 2), device_id_type=MESH)
    for s in range(LON):
        pl.semaphore_signal(barrier, inc=1, device_id=(s, b), device_id_type=MESH)
    def stage(f, first, size, sem):
        return [
            pltpu.make_async_copy(
                fields.at[f, :, pl.ds(half * ROWS + first, size), :],
                staged.at[f, :, pl.ds(half * ROWS + first, size), :],
                stage_sem.at[sem],
            )
            for half in range(2)
        ]

    def staged_wait(f, size, sem):
        both = staged.at[f, :, pl.ds(0, 2 * size), :]
        pltpu.make_async_copy(both, both, stage_sem.at[sem]).wait()

    for copy in stage(0, 0, MAIN_ROWS, 0):
        copy.start()
    mask_copy = pltpu.make_async_copy(land_mask.at[0], mask, mask_sem)
    mask_copy.start()
    for copy in stage(0, MAIN_ROWS, ROWS - MAIN_ROWS, 1):
        copy.start()
    for f in range(1, FIELDS):
        for copy in stage(f, 0, ROWS, 2):
            copy.start()
    old_copy = pltpu.make_async_copy(mean_old.at[:, 0], old, old_sem)
    old_copy.start()

    peers = []
    for dx, dy, dc in ORDER:
        level = lax.rem(x + dx, 4) * 2 + lax.rem(core + dc, 2)
        half = lax.rem(io + io // 4 + dy, 2)
        band = x * 4 + core * 2 + half
        peers.append((level, band, half, (band == io) & (level == b)))

    def send_piece(arrival, f, first, size):
        for level, band, half, here in peers:
            rows = pl.ds(pl.multiple_of(half * ROWS + first, 8), size)
            target = landed.at[f, io, pl.ds(pl.multiple_of(first, 8), size), :]

            @pl.when(jnp.logical_not(here))
            def _():
                pltpu.make_async_remote_copy(
                    src_ref=staged.at[f, level, rows, :],
                    dst_ref=target,
                    send_sem=send_sem,
                    recv_sem=recv_sem.at[arrival],
                    device_id=(band, level),
                    device_id_type=MESH,
                ).start()

            @pl.when(here)
            def _():
                pltpu.make_async_copy(fields.at[f, level, rows, :], target, recv_sem.at[arrival]).start()

    def send_early(i, carry):
        f = i // PER_FIELD
        send_piece(f, f, lax.rem(i, PER_FIELD) * MAIN_ROWS, MAIN_ROWS)
        return carry

    def send_late(i, carry):
        send_piece(LAST + i, LAST, i * MAIN_ROWS, MAIN_ROWS)
        return carry

    staged_wait(0, MAIN_ROWS, 0)
    pl.semaphore_wait(barrier, 2 * LON)
    send_early(0, 0)
    staged_wait(0, ROWS - MAIN_ROWS, 1)
    lax.fori_loop(1, PER_FIELD, send_early, 0)
    others = staged.at[pl.ds(1, FIELDS - 1)]
    pltpu.make_async_copy(others, others, stage_sem.at[2]).wait()
    lax.fori_loop(PER_FIELD, LAST * PER_FIELD, send_early, 0)
    lax.fori_loop(0, PER_FIELD - 1, send_late, 0)
    for i in range(LAST_PIECES):
        first = ROWS - MAIN_ROWS + i * LAST_ROWS
        send_piece(LAST + PER_FIELD - 1 + i, LAST, first, LAST_ROWS)

    mask_copy.wait()

    def plan(g, carry):
        plan_group(g, mask, place, arrive, count)
        return carry

    lax.fori_loop(0, GROUPS, plan, 0)
    total[...] = jnp.zeros_like(total)
    old_copy.wait()

    def pack_piece(arrival, f, first, size):
        piece = landed.at[f, :, pl.ds(pl.multiple_of(first, 8), size), :]
        pltpu.make_async_copy(piece, piece, recv_sem.at[arrival]).wait()

        def pack(k, squares):
            return squares + pack_group(f, first // 8 + k, landed, old, new, place, arrive, count)

        total[f] += lax.fori_loop(0, size // 8, pack, jnp.zeros((8, 128), jnp.float32))

    def pack_early(f, carry):
        pack_piece(f, f, 0, ROWS)
        return carry

    def pack_late(i, carry):
        pack_piece(LAST + i, LAST, i * MAIN_ROWS, MAIN_ROWS)
        return carry

    def pack_last(i, carry):
        pack_piece(LAST + PER_FIELD - 1 + i, LAST, ROWS - MAIN_ROWS + i * LAST_ROWS, LAST_ROWS)
        return carry

    lax.fori_loop(0, LAST, pack_early, 0)
    lax.fori_loop(0, PER_FIELD - 1, pack_late, 0)
    lax.fori_loop(0, LAST_PIECES, pack_last, 0)

    ocean = count[0]
    for g in range(1, GROUPS):
        ocean = ocean + count[g]
    lines = [jnp.sum(total[f], axis=0, keepdims=True) for f in range(FIELDS)]
    lines.append(jnp.sum(ocean.astype(jnp.float32), axis=0, keepdims=True))
    lines.append(jnp.zeros((1, 128), jnp.float32))
    parts[io] = jnp.concatenate(lines, axis=0)

    def send_part(s, carry):
        to = lax.rem(io + s, LON)
        pltpu.make_async_remote_copy(
            src_ref=parts.at[io],
            dst_ref=parts.at[io],
            send_sem=part_send,
            recv_sem=part_recv,
            device_id=(to, b),
            device_id_type=MESH,
        ).start()
        return carry

    lax.fori_loop(1, LON, send_part, 0)

    @pl.when(jnp.logical_not(keeps))
    def _():
        pltpu.make_async_copy(landed, landed, send_sem).wait()

    @pl.when(keeps)
    def _():
        most = landed.at[:, pl.ds(0, LON - 1)]
        pltpu.make_async_copy(most, most, send_sem).wait()

    others = parts.at[pl.ds(0, LON - 1)]
    pltpu.make_async_copy(others, others, part_send).wait()
    pltpu.make_async_copy(others, others, part_recv).wait()
    everything = parts[0]
    for s in range(1, LON):
        everything = everything + parts[s]
    sums[...] = everything


def write(new, sums, mean_new, level_rms, sem):
    for f in range(FIELDS):
        pltpu.make_async_copy(new.at[f], mean_new.at[f], sem).start()
    lane = lax.broadcasted_iota(jnp.int32, (1, 128), 1)
    square_sum = jnp.zeros((1, 128), jnp.float32)
    for f in range(FIELDS):
        field_sum = jnp.sum(sums[f : f + 1], axis=1, keepdims=True)
        square_sum = jnp.where(lane == f, field_sum, square_sum)
    ocean_total = sums[FIELDS : FIELDS + 1]
    level_rms[...] = jnp.sqrt(square_sum / ocean_total + 1e-06)[:, :FIELDS]
    pltpu.make_async_copy(new, mean_new, sem).wait()


def on_device(fields, mean_old, land_mask):
    fields, mean_old, land_mask = (
        pltpu.with_memory_space_constraint(a, pltpu.HBM) for a in (fields, mean_old, land_mask)
    )
    new, sums = pl.pallas_call(
        kernel,
        out_shape=(
            pltpu.VMEM(mean_old.shape, jnp.float32),
            pltpu.VMEM((8, 128), jnp.float32),
        ),
        in_specs=[pl.BlockSpec(memory_space=pltpu.HBM)] * 3,
        out_specs=[pl.BlockSpec(memory_space=pltpu.VMEM)] * 2,
        scratch_shapes=[
            pltpu.VMEM(fields.shape, jnp.float32),
            pltpu.VMEM((FIELDS, LON, ROWS, COLS), jnp.float32),
            pltpu.VMEM((ROWS, CHUNKS * 128), jnp.int32),
            pltpu.VMEM((FIELDS, ROWS, OUT_CHUNKS * 128), jnp.float32),
            pltpu.VMEM((GROUPS, CHUNKS * 8, 128), jnp.int32),
            pltpu.VMEM((GROUPS, CHUNKS * 8, 128), jnp.int32),
            pltpu.VMEM((GROUPS, 8, 128), jnp.int32),
            pltpu.VMEM((FIELDS, 8, 128), jnp.float32),
            pltpu.VMEM((LON, 8, 128), jnp.float32),
            pltpu.SemaphoreType.DMA((3,)),
            pltpu.SemaphoreType.DMA,
            pltpu.SemaphoreType.DMA((ARRIVALS,)),
            pltpu.SemaphoreType.DMA,
            pltpu.SemaphoreType.DMA,
            pltpu.SemaphoreType.DMA,
            pltpu.SemaphoreType.DMA,
        ],
        compiler_params=pltpu.CompilerParams(
            collective_id=0, has_side_effects=True, vmem_limit_bytes=28 * 1024 * 1024
        ),
    )(fields, mean_old, land_mask)
    mean_new, level_rms = pl.pallas_call(
        write,
        out_shape=(
            jax.ShapeDtypeStruct(mean_old.shape, jnp.float32),
            jax.ShapeDtypeStruct((1, FIELDS), jnp.float32),
        ),
        in_specs=[pl.BlockSpec(memory_space=pltpu.VMEM)] * 2,
        out_specs=(pl.BlockSpec(memory_space=pltpu.HBM), pl.BlockSpec(memory_space=pltpu.VMEM)),
        scratch_shapes=[pltpu.SemaphoreType.DMA],
        compiler_params=pltpu.CompilerParams(vmem_limit_bytes=8 * 1024 * 1024),
    )(new, sums)
    return mean_new, level_rms.reshape(FIELDS, 1)


def solution(mesh):
    in_specs = (P(None, None, "cmp", "io"), P(None, "cmp", "io", None), P("cmp", "io", None))
    out_specs = (P(None, "cmp", "io", None), P(None, "cmp"))
    return jax.shard_map(
        on_device, mesh=mesh, in_specs=in_specs, out_specs=out_specs, check_vma=False
    )
```

```python
import jax
import jax.numpy as jnp
from jax import lax
from jax.experimental import pallas as pl
from jax.experimental.pallas import tpu as pltpu
from jax.sharding import PartitionSpec as P

STEPS = 3
MESH = pl.DeviceIdType.MESH

FIELDS = 6
LON = 16
ROWS = 64
COLS = 256
CHUNKS = 32
OUT_CHUNKS = 24
GROUPS = ROWS // 8
LAST = FIELDS - 1
MAIN_ROWS, LAST_ROWS = 16, 8
PER_FIELD = ROWS // MAIN_ROWS
LAST_PIECES = MAIN_ROWS // LAST_ROWS
ARRIVALS = LAST + PER_FIELD - 1 + LAST_PIECES
ORDER = [(dx, dy, dc) for dc in (0, 1) for dx in (2, 1, 3, 0) for dy in (0, 1)]


RING_HOPS = (0, 1, 2, 1)
FAR_FIRST = sorted(
    ((dz, dy) for dz in range(4) for dy in range(4) if (dz, dy) != (0, 0)),
    key=lambda d: -RING_HOPS[d[0]] - RING_HOPS[d[1]],
)


def lanes_of(array, index):
    return jnp.take_along_axis(array, index, axis=1, mode="promise_in_bounds")


def plan_group(g, mask, place, arrive, count):
    rows = pl.ds(pl.multiple_of(g * 8, 8), 8)
    chunk = [mask[rows, pl.ds(c * 128, 128)] for c in range(CHUNKS)]
    stacked = jnp.concatenate(chunk, axis=0).astype(jnp.float32).astype(jnp.bfloat16)
    source = lax.broadcasted_iota(jnp.int32, (128, 256), 0)
    target = lax.broadcasted_iota(jnp.int32, (128, 256), 1)
    upto = ((source <= target) | (target >= 128)).astype(jnp.float32).astype(jnp.bfloat16)
    sums = jnp.dot(stacked, upto, preferred_element_type=jnp.float32).astype(jnp.int32)
    lane = lax.broadcasted_iota(jnp.int32, (8, 128), 1)
    base = jnp.zeros((8, 128), jnp.int32)
    state = []
    for c in range(CHUNKS):
        upto_here = sums[c * 8 : c * 8 + 8, :128]
        number = sums[c * 8 : c * 8 + 8, 128:]
        rank = (lane - base) & 127
        at = jnp.zeros((8, 128), jnp.int32)
        for step in (64, 32, 16, 8, 4, 2, 1):
            seen = lanes_of(upto_here, at + (step - 1))
            at = jnp.where(seen <= rank, at + step, at)
        place[g, pl.ds(c * 8, 8), :] = at
        moved = c - ((base + rank) >> 7)
        state.append(jnp.where(rank < number, moved, 0))
        base = base + number
    count[g] = base
    arrived = [jnp.zeros((8, 128), jnp.int32) for _ in range(CHUNKS)]
    for s in range(5):
        bit = 1 << s
        new_state = []
        for c in range(CHUNKS):
            kept = jnp.where((state[c] & bit) != 0, 0, state[c])
            if c + bit < CHUNKS:
                comes = (state[c + bit] & bit) != 0
                arrived[c] = jnp.where(comes, arrived[c] | bit, arrived[c])
                kept = jnp.where(comes, state[c + bit], kept)
            new_state.append(kept)
        state = new_state
    for c in range(CHUNKS):
        arrive[g, pl.ds(c * 8, 8), :] = arrived[c]


def pack_group(f, g, landed, old, new, place, arrive, count):
    rows = pl.ds(pl.multiple_of(g * 8, 8), 8)
    value = []
    for c in range(CHUNKS):
        raw = landed[f, c // 2, rows, pl.ds((c % 2) * 128, 128)]
        value.append(lanes_of(raw, place[g, pl.ds(c * 8, 8), :]))
    moves = [arrive[g, pl.ds(c * 8, 8), :] for c in range(CHUNKS)]
    for s in range(5):
        bit = 1 << s
        for c in range(CHUNKS - bit):
            if s < 4 or c < OUT_CHUNKS:
                value[c] = jnp.where((moves[c] & bit) != 0, value[c + bit], value[c])
    lane = lax.broadcasted_iota(jnp.int32, (8, 128), 1)
    left = count[g] - lane
    squares = jnp.zeros((8, 128), jnp.float32)
    for c in range(OUT_CHUNKS):
        columns = pl.ds(c * 128, 128)
        mean = (STEPS * old[f, rows, columns] + value[c]) * jnp.float32(1.0 / (STEPS + 1.0))
        mean = jnp.where(left > c * 128, mean, jnp.float32(0.0))
        new[f, 0, rows, columns] = mean
        squares = squares + mean * mean
    return squares


def kernel(
    fields, mean_old, land_mask, new, sums,
    staged, landed, mask, old, place, arrive, count, total, parts,
    stage_sem, send_sem, recv_sem, mask_sem, old_sem, part_send, part_recv,
):
    io, b = lax.axis_index("io"), lax.axis_index("cmp")
    x, core = b // 2, b % 2
    keeps = (io // 2) == b

    barrier = pltpu.get_barrier_semaphore()
    for s in range(LON):
        pl.semaphore_signal(barrier, inc=1, device_id=(s, io // 2), device_id_type=MESH)
    for s in range(LON):
        pl.semaphore_signal(barrier, inc=1, device_id=(s, b), device_id_type=MESH)
    def stage(f, first, size, sem):
        return [
            pltpu.make_async_copy(
                fields.at[f, :, pl.ds(half * ROWS + first, size), :],
                staged.at[f, :, pl.ds(half * ROWS + first, size), :],
                stage_sem.at[sem],
            )
            for half in range(2)
        ]

    def staged_wait(f, size, sem):
        both = staged.at[f, :, pl.ds(0, 2 * size), :]
        pltpu.make_async_copy(both, both, stage_sem.at[sem]).wait()

    for copy in stage(0, 0, MAIN_ROWS, 0):
        copy.start()
    mask_copy = pltpu.make_async_copy(land_mask.at[0], mask, mask_sem)
    mask_copy.start()
    for copy in stage(0, MAIN_ROWS, ROWS - MAIN_ROWS, 1):
        copy.start()
    for f in range(1, FIELDS):
        for copy in stage(f, 0, ROWS, 2):
            copy.start()
    old_copy = pltpu.make_async_copy(mean_old.at[:, 0], old, old_sem)
    old_copy.start()

    peers = []
    for dx, dy, dc in ORDER:
        level = lax.rem(x + dx, 4) * 2 + lax.rem(core + dc, 2)
        half = lax.rem((lax.rem(io, 4) + 1) // 2 + 1 + core + dy, 2)
        band = x * 4 + core * 2 + half
        peers.append((level, band, half, (band == io) & (level == b)))

    def send_piece(arrival, f, first, size):
        for level, band, half, here in peers:
            rows = pl.ds(pl.multiple_of(half * ROWS + first, 8), size)
            target = landed.at[f, io, pl.ds(pl.multiple_of(first, 8), size), :]

            @pl.when(jnp.logical_not(here))
            def _():
                pltpu.make_async_remote_copy(
                    src_ref=staged.at[f, level, rows, :],
                    dst_ref=target,
                    send_sem=send_sem,
                    recv_sem=recv_sem.at[arrival],
                    device_id=(band, level),
                    device_id_type=MESH,
                ).start()

            @pl.when(here)
            def _():
                pltpu.make_async_copy(fields.at[f, level, rows, :], target, recv_sem.at[arrival]).start()

    def send_early(i, carry):
        f = i // PER_FIELD
        send_piece(f, f, lax.rem(i, PER_FIELD) * MAIN_ROWS, MAIN_ROWS)
        return carry

    def send_late(i, carry):
        send_piece(LAST + i, LAST, i * MAIN_ROWS, MAIN_ROWS)
        return carry

    staged_wait(0, MAIN_ROWS, 0)
    pl.semaphore_wait(barrier, 2 * LON)
    send_early(0, 0)
    staged_wait(0, ROWS - MAIN_ROWS, 1)
    lax.fori_loop(1, PER_FIELD, send_early, 0)
    others = staged.at[pl.ds(1, FIELDS - 1)]
    pltpu.make_async_copy(others, others, stage_sem.at[2]).wait()
    lax.fori_loop(PER_FIELD, LAST * PER_FIELD, send_early, 0)
    lax.fori_loop(0, PER_FIELD - 1, send_late, 0)
    for i in range(LAST_PIECES):
        first = ROWS - MAIN_ROWS + i * LAST_ROWS
        send_piece(LAST + PER_FIELD - 1 + i, LAST, first, LAST_ROWS)

    mask_copy.wait()

    def plan(g, carry):
        plan_group(g, mask, place, arrive, count)
        return carry

    lax.fori_loop(0, GROUPS, plan, 0)
    total[...] = jnp.zeros_like(total)
    old_copy.wait()

    def pack_piece(arrival, f, first, size):
        piece = landed.at[f, :, pl.ds(pl.multiple_of(first, 8), size), :]
        pltpu.make_async_copy(piece, piece, recv_sem.at[arrival]).wait()

        def pack(k, squares):
            return squares + pack_group(f, first // 8 + k, landed, old, new, place, arrive, count)

        total[f] += lax.fori_loop(0, size // 8, pack, jnp.zeros((8, 128), jnp.float32))

    def pack_early(f, carry):
        pack_piece(f, f, 0, ROWS)
        return carry

    def pack_late(i, carry):
        pack_piece(LAST + i, LAST, i * MAIN_ROWS, MAIN_ROWS)
        return carry

    def pack_last(i, carry):
        pack_piece(LAST + PER_FIELD - 1 + i, LAST, ROWS - MAIN_ROWS + i * LAST_ROWS, LAST_ROWS)
        return carry

    lax.fori_loop(0, LAST, pack_early, 0)
    lax.fori_loop(0, PER_FIELD - 1, pack_late, 0)
    lax.fori_loop(0, LAST_PIECES, pack_last, 0)

    ocean = count[0]
    for g in range(1, GROUPS):
        ocean = ocean + count[g]
    lines = [jnp.sum(total[f], axis=0, keepdims=True) for f in range(FIELDS)]
    lines.append(jnp.sum(ocean.astype(jnp.float32), axis=0, keepdims=True))
    lines.append(jnp.zeros((1, 128), jnp.float32))
    parts[io] = jnp.concatenate(lines, axis=0)

    for dz, dy in FAR_FIRST:
        to = lax.rem(io // 4 + dz, 4) * 4 + lax.rem(lax.rem(io, 4) + dy, 4)
        pltpu.make_async_remote_copy(
            src_ref=parts.at[io],
            dst_ref=parts.at[io],
            send_sem=part_send,
            recv_sem=part_recv,
            device_id=(to, b),
            device_id_type=MESH,
        ).start()

    @pl.when(jnp.logical_not(keeps))
    def _():
        pltpu.make_async_copy(landed, landed, send_sem).wait()

    @pl.when(keeps)
    def _():
        most = landed.at[:, pl.ds(0, LON - 1)]
        pltpu.make_async_copy(most, most, send_sem).wait()

    others = parts.at[pl.ds(0, LON - 1)]
    pltpu.make_async_copy(others, others, part_send).wait()
    pltpu.make_async_copy(others, others, part_recv).wait()
    everything = parts[0]
    for s in range(1, LON):
        everything = everything + parts[s]
    sums[...] = everything


def write(new, sums, mean_new, level_rms, row, mean_sem, row_sem):
    for f in range(FIELDS):
        pltpu.make_async_copy(new.at[f], mean_new.at[f], mean_sem).start()
    lane = lax.broadcasted_iota(jnp.int32, (1, 128), 1)
    square_sum = jnp.zeros((1, 128), jnp.float32)
    for f in range(FIELDS):
        field_sum = jnp.sum(sums[f : f + 1], axis=1, keepdims=True)
        square_sum = jnp.where(lane == f, field_sum, square_sum)
    ocean_total = sums[FIELDS : FIELDS + 1]
    row[...] = jnp.sqrt(square_sum / ocean_total + 1e-06)[:, :FIELDS]
    row_copy = pltpu.make_async_copy(row, level_rms, row_sem)
    row_copy.start()
    pltpu.make_async_copy(new, mean_new, mean_sem).wait()
    row_copy.wait()


def on_device(fields, mean_old, land_mask):
    fields, mean_old, land_mask = (
        pltpu.with_memory_space_constraint(a, pltpu.HBM) for a in (fields, mean_old, land_mask)
    )
    new, sums = pl.pallas_call(
        kernel,
        out_shape=(
            pltpu.VMEM(mean_old.shape, jnp.float32),
            pltpu.VMEM((8, 128), jnp.float32),
        ),
        in_specs=[pl.BlockSpec(memory_space=pltpu.HBM)] * 3,
        out_specs=[pl.BlockSpec(memory_space=pltpu.VMEM)] * 2,
        scratch_shapes=[
            pltpu.VMEM(fields.shape, jnp.float32),
            pltpu.VMEM((FIELDS, LON, ROWS, COLS), jnp.float32),
            pltpu.VMEM((ROWS, CHUNKS * 128), jnp.int32),
            pltpu.VMEM((FIELDS, ROWS, OUT_CHUNKS * 128), jnp.float32),
            pltpu.VMEM((GROUPS, CHUNKS * 8, 128), jnp.int32),
            pltpu.VMEM((GROUPS, CHUNKS * 8, 128), jnp.int32),
            pltpu.VMEM((GROUPS, 8, 128), jnp.int32),
            pltpu.VMEM((FIELDS, 8, 128), jnp.float32),
            pltpu.VMEM((LON, 8, 128), jnp.float32),
            pltpu.SemaphoreType.DMA((3,)),
            pltpu.SemaphoreType.DMA,
            pltpu.SemaphoreType.DMA((ARRIVALS,)),
            pltpu.SemaphoreType.DMA,
            pltpu.SemaphoreType.DMA,
            pltpu.SemaphoreType.DMA,
            pltpu.SemaphoreType.DMA,
        ],
        compiler_params=pltpu.CompilerParams(
            collective_id=0, has_side_effects=True, vmem_limit_bytes=28 * 1024 * 1024
        ),
    )(fields, mean_old, land_mask)
    mean_new, level_rms = pl.pallas_call(
        write,
        out_shape=(
            jax.ShapeDtypeStruct(mean_old.shape, jnp.float32),
            jax.ShapeDtypeStruct((1, FIELDS), jnp.float32),
        ),
        in_specs=[pl.BlockSpec(memory_space=pltpu.VMEM)] * 2,
        out_specs=[pl.BlockSpec(memory_space=pltpu.HBM)] * 2,
        scratch_shapes=[
            pltpu.VMEM((1, FIELDS), jnp.float32),
            pltpu.SemaphoreType.DMA,
            pltpu.SemaphoreType.DMA,
        ],
        compiler_params=pltpu.CompilerParams(vmem_limit_bytes=8 * 1024 * 1024),
    )(new, sums)
    return mean_new, level_rms.reshape(FIELDS, 1)


def solution(mesh):
    in_specs = (P(None, None, "cmp", "io"), P(None, "cmp", "io", None), P("cmp", "io", None))
    out_specs = (P(None, "cmp", "io", None), P(None, "cmp"))
    return jax.shard_map(
        on_device, mesh=mesh, in_specs=in_specs, out_specs=out_specs, check_vma=False
    )
```

```python
import jax
import jax.numpy as jnp
from jax import lax
from jax.experimental import pallas as pl
from jax.experimental.pallas import tpu as pltpu
from jax.sharding import PartitionSpec as P

STEPS = 3
MESH = pl.DeviceIdType.MESH

FIELDS = 6
LON = 16
ROWS = 64
COLS = 256
CHUNKS = 32
OUT_CHUNKS = 24
GROUPS = ROWS // 8
LAST = FIELDS - 1
MAIN_ROWS, LAST_ROWS = 16, 8
PER_FIELD = ROWS // MAIN_ROWS
LAST_PIECES = MAIN_ROWS // LAST_ROWS
ARRIVALS = LAST + PER_FIELD - 1 + LAST_PIECES
ORDER = [(dx, dy, dc) for dc in (0, 1) for dx in (2, 1, 3, 0) for dy in (0, 1)]


RING_HOPS = (0, 1, 2, 1)
FAR_FIRST = sorted(
    ((dz, dy) for dz in range(4) for dy in range(4) if (dz, dy) != (0, 0)),
    key=lambda d: -RING_HOPS[d[0]] - RING_HOPS[d[1]],
)


def lanes_of(array, index):
    return jnp.take_along_axis(array, index, axis=1, mode="promise_in_bounds")


def plan_group(g, mask, place, arrive, count):
    rows = pl.ds(pl.multiple_of(g * 8, 8), 8)
    chunk = [mask[rows, pl.ds(c * 128, 128)] for c in range(CHUNKS)]
    stacked = jnp.concatenate(chunk, axis=0).astype(jnp.float32).astype(jnp.bfloat16)
    source = lax.broadcasted_iota(jnp.int32, (128, 256), 0)
    target = lax.broadcasted_iota(jnp.int32, (128, 256), 1)
    upto = ((source <= target) | (target >= 128)).astype(jnp.float32).astype(jnp.bfloat16)
    sums = jnp.dot(stacked, upto, preferred_element_type=jnp.float32).astype(jnp.int32)
    lane = lax.broadcasted_iota(jnp.int32, (8, 128), 1)
    base = jnp.zeros((8, 128), jnp.int32)
    state = []
    for c in range(CHUNKS):
        upto_here = sums[c * 8 : c * 8 + 8, :128]
        number = sums[c * 8 : c * 8 + 8, 128:]
        rank = (lane - base) & 127
        at = jnp.zeros((8, 128), jnp.int32)
        for step in (64, 32, 16, 8, 4, 2, 1):
            seen = lanes_of(upto_here, at + (step - 1))
            at = jnp.where(seen <= rank, at + step, at)
        place[g, pl.ds(c * 8, 8), :] = at
        moved = c - ((base + rank) >> 7)
        state.append(jnp.where(rank < number, moved, 0))
        base = base + number
    count[g] = base
    arrived = [jnp.zeros((8, 128), jnp.int32) for _ in range(CHUNKS)]
    for s in range(5):
        bit = 1 << s
        new_state = []
        for c in range(CHUNKS):
            kept = jnp.where((state[c] & bit) != 0, 0, state[c])
            if c + bit < CHUNKS:
                comes = (state[c + bit] & bit) != 0
                arrived[c] = jnp.where(comes, arrived[c] | bit, arrived[c])
                kept = jnp.where(comes, state[c + bit], kept)
            new_state.append(kept)
        state = new_state
    for c in range(CHUNKS):
        arrive[g, pl.ds(c * 8, 8), :] = arrived[c]


def pack_group(f, g, landed, old, new, place, arrive, count):
    rows = pl.ds(pl.multiple_of(g * 8, 8), 8)
    value = []
    for c in range(CHUNKS):
        raw = landed[f, c // 2, rows, pl.ds((c % 2) * 128, 128)]
        value.append(lanes_of(raw, place[g, pl.ds(c * 8, 8), :]))
    moves = [arrive[g, pl.ds(c * 8, 8), :] for c in range(CHUNKS)]
    for s in range(5):
        bit = 1 << s
        for c in range(CHUNKS - bit):
            if s < 4 or c < OUT_CHUNKS:
                value[c] = jnp.where((moves[c] & bit) != 0, value[c + bit], value[c])
    lane = lax.broadcasted_iota(jnp.int32, (8, 128), 1)
    left = count[g] - lane
    squares = jnp.zeros((8, 128), jnp.float32)
    for c in range(OUT_CHUNKS):
        columns = pl.ds(c * 128, 128)
        mean = (STEPS * old[f, rows, columns] + value[c]) * jnp.float32(1.0 / (STEPS + 1.0))
        mean = jnp.where(left > c * 128, mean, jnp.float32(0.0))
        new[f, 0, rows, columns] = mean
        squares = squares + mean * mean
    return squares


def kernel(
    fields, mean_old, land_mask, new, sums,
    staged, landed, mask, old, place, arrive, count, total, parts,
    stage_sem, send_sem, recv_sem, mask_sem, old_sem, part_send, part_recv, group_sem,
):
    io, b = lax.axis_index("io"), lax.axis_index("cmp")
    x, core = b // 2, b % 2
    keeps = (io // 2) == b

    barrier = pltpu.get_barrier_semaphore()
    for s in range(LON):
        pl.semaphore_signal(barrier, inc=1, device_id=(s, io // 2), device_id_type=MESH)
    def stage(f, first, size, sem):
        return [
            pltpu.make_async_copy(
                fields.at[f, :, pl.ds(half * ROWS + first, size), :],
                staged.at[f, :, pl.ds(half * ROWS + first, size), :],
                stage_sem.at[sem],
            )
            for half in range(2)
        ]

    def staged_wait(f, size, sem):
        both = staged.at[f, :, pl.ds(0, 2 * size), :]
        pltpu.make_async_copy(both, both, stage_sem.at[sem]).wait()

    for copy in stage(0, 0, MAIN_ROWS, 0):
        copy.start()
    mask_copy = pltpu.make_async_copy(land_mask.at[0], mask, mask_sem)
    mask_copy.start()
    for copy in stage(0, MAIN_ROWS, ROWS - MAIN_ROWS, 1):
        copy.start()
    for f in range(1, FIELDS):
        for copy in stage(f, 0, ROWS, 2):
            copy.start()
    old_copy = pltpu.make_async_copy(mean_old.at[:, 0], old, old_sem)
    old_copy.start()

    peers = []
    for dx, dy, dc in ORDER:
        level = lax.rem(x + dx, 4) * 2 + lax.rem(core + dc, 2)
        half = lax.rem((lax.rem(io, 4) + 1) // 2 + 1 + core + dy, 2)
        band = x * 4 + core * 2 + half
        peers.append((level, band, half, (band == io) & (level == b)))

    def send_piece(arrival, f, first, size):
        for level, band, half, here in peers:
            rows = pl.ds(pl.multiple_of(half * ROWS + first, 8), size)
            target = landed.at[f, io, pl.ds(pl.multiple_of(first, 8), size), :]

            @pl.when(jnp.logical_not(here))
            def _():
                pltpu.make_async_remote_copy(
                    src_ref=staged.at[f, level, rows, :],
                    dst_ref=target,
                    send_sem=send_sem,
                    recv_sem=recv_sem.at[arrival],
                    device_id=(band, level),
                    device_id_type=MESH,
                ).start()

            @pl.when(here)
            def _():
                pltpu.make_async_copy(fields.at[f, level, rows, :], target, recv_sem.at[arrival]).start()

    def send_early(i, carry):
        f = i // PER_FIELD
        send_piece(f, f, lax.rem(i, PER_FIELD) * MAIN_ROWS, MAIN_ROWS)
        return carry

    def send_late(i, carry):
        send_piece(LAST + i, LAST, i * MAIN_ROWS, MAIN_ROWS)
        return carry

    staged_wait(0, MAIN_ROWS, 0)
    pl.semaphore_wait(barrier, LON)
    send_early(0, 0)
    staged_wait(0, ROWS - MAIN_ROWS, 1)
    lax.fori_loop(1, PER_FIELD, send_early, 0)
    others = staged.at[pl.ds(1, FIELDS - 1)]
    pltpu.make_async_copy(others, others, stage_sem.at[2]).wait()
    lax.fori_loop(PER_FIELD, LAST * PER_FIELD, send_early, 0)
    lax.fori_loop(0, PER_FIELD - 1, send_late, 0)
    for i in range(LAST_PIECES):
        first = ROWS - MAIN_ROWS + i * LAST_ROWS
        send_piece(LAST + PER_FIELD - 1 + i, LAST, first, LAST_ROWS)

    mask_copy.wait()

    def plan(g, carry):
        plan_group(g, mask, place, arrive, count)
        return carry

    lax.fori_loop(0, GROUPS, plan, 0)
    total[...] = jnp.zeros_like(total)
    old_copy.wait()

    def pack_piece(arrival, f, first, size):
        piece = landed.at[f, :, pl.ds(pl.multiple_of(first, 8), size), :]
        pltpu.make_async_copy(piece, piece, recv_sem.at[arrival]).wait()

        def pack(k, squares):
            return squares + pack_group(f, first // 8 + k, landed, old, new, place, arrive, count)

        total[f] += lax.fori_loop(0, size // 8, pack, jnp.zeros((8, 128), jnp.float32))

    def pack_early(f, carry):
        pack_piece(f, f, 0, ROWS)
        return carry

    def pack_late(i, carry):
        pack_piece(LAST + i, LAST, i * MAIN_ROWS, MAIN_ROWS)
        return carry

    def pack_last(i, carry):
        pack_piece(LAST + PER_FIELD - 1 + i, LAST, ROWS - MAIN_ROWS + i * LAST_ROWS, LAST_ROWS)
        return carry

    pack_early(0, 0)

    @pl.when(io == 2 * b)
    def _():
        for s in range(LON):
            pl.semaphore_signal(group_sem, inc=1, device_id=(s, b), device_id_type=MESH)

    lax.fori_loop(1, LAST, pack_early, 0)
    lax.fori_loop(0, PER_FIELD - 1, pack_late, 0)
    lax.fori_loop(0, LAST_PIECES, pack_last, 0)

    ocean = count[0]
    for g in range(1, GROUPS):
        ocean = ocean + count[g]
    lines = [jnp.sum(total[f], axis=0, keepdims=True) for f in range(FIELDS)]
    lines.append(jnp.sum(ocean.astype(jnp.float32), axis=0, keepdims=True))
    lines.append(jnp.zeros((1, 128), jnp.float32))
    parts[io] = jnp.concatenate(lines, axis=0)

    pl.semaphore_wait(group_sem, 1)
    for dz, dy in FAR_FIRST:
        to = lax.rem(io // 4 + dz, 4) * 4 + lax.rem(lax.rem(io, 4) + dy, 4)
        pltpu.make_async_remote_copy(
            src_ref=parts.at[io],
            dst_ref=parts.at[io],
            send_sem=part_send,
            recv_sem=part_recv,
            device_id=(to, b),
            device_id_type=MESH,
        ).start()

    @pl.when(jnp.logical_not(keeps))
    def _():
        pltpu.make_async_copy(landed, landed, send_sem).wait()

    @pl.when(keeps)
    def _():
        most = landed.at[:, pl.ds(0, LON - 1)]
        pltpu.make_async_copy(most, most, send_sem).wait()

    others = parts.at[pl.ds(0, LON - 1)]
    pltpu.make_async_copy(others, others, part_send).wait()
    pltpu.make_async_copy(others, others, part_recv).wait()
    everything = parts[0]
    for s in range(1, LON):
        everything = everything + parts[s]
    sums[...] = everything


def write(new, sums, mean_new, level_rms, row, mean_sem, row_sem):
    for f in range(FIELDS):
        pltpu.make_async_copy(new.at[f], mean_new.at[f], mean_sem).start()
    lane = lax.broadcasted_iota(jnp.int32, (1, 128), 1)
    square_sum = jnp.zeros((1, 128), jnp.float32)
    for f in range(FIELDS):
        field_sum = jnp.sum(sums[f : f + 1], axis=1, keepdims=True)
        square_sum = jnp.where(lane == f, field_sum, square_sum)
    ocean_total = sums[FIELDS : FIELDS + 1]
    row[...] = jnp.sqrt(square_sum / ocean_total + 1e-06)[:, :FIELDS]
    row_copy = pltpu.make_async_copy(row, level_rms, row_sem)
    row_copy.start()
    pltpu.make_async_copy(new, mean_new, mean_sem).wait()
    row_copy.wait()


def on_device(fields, mean_old, land_mask):
    fields, mean_old, land_mask = (
        pltpu.with_memory_space_constraint(a, pltpu.HBM) for a in (fields, mean_old, land_mask)
    )
    new, sums = pl.pallas_call(
        kernel,
        out_shape=(
            pltpu.VMEM(mean_old.shape, jnp.float32),
            pltpu.VMEM((8, 128), jnp.float32),
        ),
        in_specs=[pl.BlockSpec(memory_space=pltpu.HBM)] * 3,
        out_specs=[pl.BlockSpec(memory_space=pltpu.VMEM)] * 2,
        scratch_shapes=[
            pltpu.VMEM(fields.shape, jnp.float32),
            pltpu.VMEM((FIELDS, LON, ROWS, COLS), jnp.float32),
            pltpu.VMEM((ROWS, CHUNKS * 128), jnp.int32),
            pltpu.VMEM((FIELDS, ROWS, OUT_CHUNKS * 128), jnp.float32),
            pltpu.VMEM((GROUPS, CHUNKS * 8, 128), jnp.int32),
            pltpu.VMEM((GROUPS, CHUNKS * 8, 128), jnp.int32),
            pltpu.VMEM((GROUPS, 8, 128), jnp.int32),
            pltpu.VMEM((FIELDS, 8, 128), jnp.float32),
            pltpu.VMEM((LON, 8, 128), jnp.float32),
            pltpu.SemaphoreType.DMA((3,)),
            pltpu.SemaphoreType.DMA,
            pltpu.SemaphoreType.DMA((ARRIVALS,)),
            pltpu.SemaphoreType.DMA,
            pltpu.SemaphoreType.DMA,
            pltpu.SemaphoreType.DMA,
            pltpu.SemaphoreType.DMA,
            pltpu.SemaphoreType.REGULAR,
        ],
        compiler_params=pltpu.CompilerParams(
            collective_id=0, has_side_effects=True, vmem_limit_bytes=28 * 1024 * 1024
        ),
    )(fields, mean_old, land_mask)
    mean_new, level_rms = pl.pallas_call(
        write,
        out_shape=(
            jax.ShapeDtypeStruct(mean_old.shape, jnp.float32),
            jax.ShapeDtypeStruct((1, FIELDS), jnp.float32),
        ),
        in_specs=[pl.BlockSpec(memory_space=pltpu.VMEM)] * 2,
        out_specs=[pl.BlockSpec(memory_space=pltpu.HBM)] * 2,
        scratch_shapes=[
            pltpu.VMEM((1, FIELDS), jnp.float32),
            pltpu.SemaphoreType.DMA,
            pltpu.SemaphoreType.DMA,
        ],
        compiler_params=pltpu.CompilerParams(vmem_limit_bytes=8 * 1024 * 1024),
    )(new, sums)
    return mean_new, level_rms.reshape(FIELDS, 1)


def solution(mesh):
    in_specs = (P(None, None, "cmp", "io"), P(None, "cmp", "io", None), P("cmp", "io", None))
    out_specs = (P(None, "cmp", "io", None), P(None, "cmp"))
    return jax.shard_map(
        on_device, mesh=mesh, in_specs=in_specs, out_specs=out_specs, check_vma=False
    )
```

```python
import jax
import jax.numpy as jnp
from jax import lax
from jax.experimental import pallas as pl
from jax.experimental.pallas import tpu as pltpu
from jax.sharding import PartitionSpec as P

STEPS = 3
MESH = pl.DeviceIdType.MESH

FIELDS = 6
LON = 16
ROWS = 64
COLS = 256
CHUNKS = 32
OUT_CHUNKS = 24
GROUPS = ROWS // 8
LAST = FIELDS - 1
PIECE_ROWS = 8
PER_FIELD = ROWS // PIECE_ROWS
LATE = ((0, 32), (32, 16), (48, 8), (56, 8))
ARRIVALS = LAST + len(LATE)
ORDER = [(dx, dy, dc) for dc in (0, 1) for dx in (2, 1, 3, 0) for dy in (0, 1)]


RING_HOPS = (0, 1, 2, 1)
FAR_FIRST = sorted(
    ((dz, dy) for dz in range(4) for dy in range(4) if (dz, dy) != (0, 0)),
    key=lambda d: -RING_HOPS[d[0]] - RING_HOPS[d[1]],
)


def band_at(io, dz, dy):
    return lax.rem(io // 4 + dz, 4) * 4 + lax.rem(lax.rem(io, 4) + dy, 4)


def at_eight(row):
    return row if isinstance(row, int) else pl.multiple_of(row, 8)


def lanes_of(array, index):
    return jnp.take_along_axis(array, index, axis=1, mode="promise_in_bounds")


def plan_group(g, mask, place, arrive, count):
    rows = pl.ds(pl.multiple_of(g * 8, 8), 8)
    chunk = [mask[rows, pl.ds(c * 128, 128)] for c in range(CHUNKS)]
    stacked = jnp.concatenate(chunk, axis=0).astype(jnp.float32).astype(jnp.bfloat16)
    source = lax.broadcasted_iota(jnp.int32, (128, 256), 0)
    target = lax.broadcasted_iota(jnp.int32, (128, 256), 1)
    upto = ((source <= target) | (target >= 128)).astype(jnp.float32).astype(jnp.bfloat16)
    sums = jnp.dot(stacked, upto, preferred_element_type=jnp.float32).astype(jnp.int32)
    lane = lax.broadcasted_iota(jnp.int32, (8, 128), 1)
    base = jnp.zeros((8, 128), jnp.int32)
    state = []
    for c in range(CHUNKS):
        upto_here = sums[c * 8 : c * 8 + 8, :128]
        number = sums[c * 8 : c * 8 + 8, 128:]
        rank = (lane - base) & 127
        at = jnp.zeros((8, 128), jnp.int32)
        for step in (64, 32, 16, 8, 4, 2, 1):
            seen = lanes_of(upto_here, at + (step - 1))
            at = jnp.where(seen <= rank, at + step, at)
        place[g, pl.ds(c * 8, 8), :] = at
        moved = c - ((base + rank) >> 7)
        state.append(jnp.where(rank < number, moved, 0))
        base = base + number
    count[g] = base
    arrived = [jnp.zeros((8, 128), jnp.int32) for _ in range(CHUNKS)]
    for s in range(5):
        bit = 1 << s
        new_state = []
        for c in range(CHUNKS):
            kept = jnp.where((state[c] & bit) != 0, 0, state[c])
            if c + bit < CHUNKS:
                comes = (state[c + bit] & bit) != 0
                arrived[c] = jnp.where(comes, arrived[c] | bit, arrived[c])
                kept = jnp.where(comes, state[c + bit], kept)
            new_state.append(kept)
        state = new_state
    for c in range(CHUNKS):
        arrive[g, pl.ds(c * 8, 8), :] = arrived[c]


def pack_group(f, g, landed, old, new, place, arrive, count):
    rows = pl.ds(pl.multiple_of(g * 8, 8), 8)
    value = []
    for c in range(CHUNKS):
        raw = landed[f, c // 2, rows, pl.ds((c % 2) * 128, 128)]
        value.append(lanes_of(raw, place[g, pl.ds(c * 8, 8), :]))
    moves = [arrive[g, pl.ds(c * 8, 8), :] for c in range(CHUNKS)]
    for s in range(5):
        bit = 1 << s
        for c in range(CHUNKS - bit):
            if s < 4 or c < OUT_CHUNKS:
                value[c] = jnp.where((moves[c] & bit) != 0, value[c + bit], value[c])
    lane = lax.broadcasted_iota(jnp.int32, (8, 128), 1)
    left = count[g] - lane
    squares = jnp.zeros((8, 128), jnp.float32)
    for c in range(OUT_CHUNKS):
        columns = pl.ds(c * 128, 128)
        mean = (STEPS * old[f, rows, columns] + value[c]) * jnp.float32(1.0 / (STEPS + 1.0))
        mean = jnp.where(left > c * 128, mean, jnp.float32(0.0))
        new[f, 0, rows, columns] = mean
        squares = squares + mean * mean
    return squares


def kernel(
    fields, mean_old, land_mask, new, sums,
    staged, landed, mask, old, place, arrive, count, total, parts,
    stage_sem, send_sem, recv_sem, mask_sem, old_sem, part_send, part_recv, group_sem,
):
    io, b = lax.axis_index("io"), lax.axis_index("cmp")
    x, core = b // 2, b % 2
    keeps = (io // 2) == b

    barrier = pltpu.get_barrier_semaphore()
    for dz, dy in FAR_FIRST + [(0, 0)]:
        pl.semaphore_signal(
            barrier, inc=1, device_id=(band_at(io, dz, dy), io // 2), device_id_type=MESH
        )
    def stage(f, first, size, sem):
        return [
            pltpu.make_async_copy(
                fields.at[f, :, pl.ds(half * ROWS + first, size), :],
                staged.at[f, :, pl.ds(half * ROWS + first, size), :],
                stage_sem.at[sem],
            )
            for half in range(2)
        ]

    def staged_wait(f, size, sem):
        both = staged.at[f, :, pl.ds(0, 2 * size), :]
        pltpu.make_async_copy(both, both, stage_sem.at[sem]).wait()

    for copy in stage(0, 0, PIECE_ROWS, 0):
        copy.start()
    mask_copy = pltpu.make_async_copy(land_mask.at[0], mask, mask_sem)
    mask_copy.start()
    for copy in stage(0, PIECE_ROWS, ROWS - PIECE_ROWS, 1):
        copy.start()
    for f in range(1, FIELDS):
        for copy in stage(f, 0, ROWS, 2):
            copy.start()
    old_copy = pltpu.make_async_copy(mean_old.at[:, 0], old, old_sem)
    old_copy.start()

    peers = []
    for dx, dy, dc in ORDER:
        level = lax.rem(x + dx, 4) * 2 + lax.rem(core + dc, 2)
        half = lax.rem((lax.rem(io, 4) + 1) // 2 + 1 + core + dy, 2)
        band = x * 4 + core * 2 + half
        peers.append((level, band, half, (band == io) & (level == b)))

    def send_piece(arrival, f, first, size):
        for level, band, half, here in peers:
            rows = pl.ds(pl.multiple_of(half * ROWS + first, 8), size)
            target = landed.at[f, io, pl.ds(at_eight(first), size), :]

            @pl.when(jnp.logical_not(here))
            def _():
                pltpu.make_async_remote_copy(
                    src_ref=staged.at[f, level, rows, :],
                    dst_ref=target,
                    send_sem=send_sem,
                    recv_sem=recv_sem.at[arrival],
                    device_id=(band, level),
                    device_id_type=MESH,
                ).start()

            @pl.when(here)
            def _():
                pltpu.make_async_copy(fields.at[f, level, rows, :], target, recv_sem.at[arrival]).start()

    def send_early(i, carry):
        f = i // PER_FIELD
        send_piece(f, f, lax.rem(i, PER_FIELD) * PIECE_ROWS, PIECE_ROWS)
        return carry

    staged_wait(0, PIECE_ROWS, 0)
    pl.semaphore_wait(barrier, LON)
    send_early(0, 0)
    staged_wait(0, ROWS - PIECE_ROWS, 1)
    lax.fori_loop(1, PER_FIELD, send_early, 0)
    others = staged.at[pl.ds(1, FIELDS - 1)]
    pltpu.make_async_copy(others, others, stage_sem.at[2]).wait()
    lax.fori_loop(PER_FIELD, LAST * PER_FIELD, send_early, 0)
    for k, (start, size) in enumerate(LATE):

        def send_late(i, carry, k=k, start=start):
            send_piece(LAST + k, LAST, start + i * PIECE_ROWS, PIECE_ROWS)
            return carry

        lax.fori_loop(0, size // PIECE_ROWS, send_late, 0)

    mask_copy.wait()

    def plan(g, carry):
        plan_group(g, mask, place, arrive, count)
        return carry

    lax.fori_loop(0, GROUPS, plan, 0)
    total[...] = jnp.zeros_like(total)
    old_copy.wait()

    def pack_piece(arrival, f, first, size):
        piece = landed.at[f, :, pl.ds(at_eight(first), size), :]
        pltpu.make_async_copy(piece, piece, recv_sem.at[arrival]).wait()

        def pack(k, squares):
            return squares + pack_group(f, first // 8 + k, landed, old, new, place, arrive, count)

        total[f] += lax.fori_loop(0, size // 8, pack, jnp.zeros((8, 128), jnp.float32))

    def pack_early(f, carry):
        pack_piece(f, f, 0, ROWS)
        return carry

    pack_early(0, 0)

    @pl.when(io == 2 * b)
    def _():
        for s in range(LON):
            pl.semaphore_signal(group_sem, inc=1, device_id=(s, b), device_id_type=MESH)

    lax.fori_loop(1, LAST, pack_early, 0)
    for k, (start, size) in enumerate(LATE):
        pack_piece(LAST + k, LAST, start, size)

    ocean = count[0]
    for g in range(1, GROUPS):
        ocean = ocean + count[g]
    lines = [jnp.sum(total[f], axis=0, keepdims=True) for f in range(FIELDS)]
    lines.append(jnp.sum(ocean.astype(jnp.float32), axis=0, keepdims=True))
    lines.append(jnp.zeros((1, 128), jnp.float32))
    parts[io] = jnp.concatenate(lines, axis=0)

    pl.semaphore_wait(group_sem, 1)
    for dz, dy in FAR_FIRST:
        pltpu.make_async_remote_copy(
            src_ref=parts.at[io],
            dst_ref=parts.at[io],
            send_sem=part_send,
            recv_sem=part_recv,
            device_id=(band_at(io, dz, dy), b),
            device_id_type=MESH,
        ).start()

    @pl.when(jnp.logical_not(keeps))
    def _():
        pltpu.make_async_copy(landed, landed, send_sem).wait()

    @pl.when(keeps)
    def _():
        most = landed.at[:, pl.ds(0, LON - 1)]
        pltpu.make_async_copy(most, most, send_sem).wait()

    others = parts.at[pl.ds(0, LON - 1)]
    pltpu.make_async_copy(others, others, part_send).wait()
    pltpu.make_async_copy(others, others, part_recv).wait()
    everything = parts[0]
    for s in range(1, LON):
        everything = everything + parts[s]
    sums[...] = everything


def write(new, sums, mean_new, level_rms, row, mean_sem, row_sem):
    for f in range(FIELDS):
        pltpu.make_async_copy(new.at[f], mean_new.at[f], mean_sem).start()
    lane = lax.broadcasted_iota(jnp.int32, (1, 128), 1)
    square_sum = jnp.zeros((1, 128), jnp.float32)
    for f in range(FIELDS):
        field_sum = jnp.sum(sums[f : f + 1], axis=1, keepdims=True)
        square_sum = jnp.where(lane == f, field_sum, square_sum)
    ocean_total = sums[FIELDS : FIELDS + 1]
    row[...] = jnp.sqrt(square_sum / ocean_total + 1e-06)[:, :FIELDS]
    row_copy = pltpu.make_async_copy(row, level_rms, row_sem)
    row_copy.start()
    pltpu.make_async_copy(new, mean_new, mean_sem).wait()
    row_copy.wait()


def on_device(fields, mean_old, land_mask):
    fields, mean_old, land_mask = (
        pltpu.with_memory_space_constraint(a, pltpu.HBM) for a in (fields, mean_old, land_mask)
    )
    new, sums = pl.pallas_call(
        kernel,
        out_shape=(
            pltpu.VMEM(mean_old.shape, jnp.float32),
            pltpu.VMEM((8, 128), jnp.float32),
        ),
        in_specs=[pl.BlockSpec(memory_space=pltpu.HBM)] * 3,
        out_specs=[pl.BlockSpec(memory_space=pltpu.VMEM)] * 2,
        scratch_shapes=[
            pltpu.VMEM(fields.shape, jnp.float32),
            pltpu.VMEM((FIELDS, LON, ROWS, COLS), jnp.float32),
            pltpu.VMEM((ROWS, CHUNKS * 128), jnp.int32),
            pltpu.VMEM((FIELDS, ROWS, OUT_CHUNKS * 128), jnp.float32),
            pltpu.VMEM((GROUPS, CHUNKS * 8, 128), jnp.int32),
            pltpu.VMEM((GROUPS, CHUNKS * 8, 128), jnp.int32),
            pltpu.VMEM((GROUPS, 8, 128), jnp.int32),
            pltpu.VMEM((FIELDS, 8, 128), jnp.float32),
            pltpu.VMEM((LON, 8, 128), jnp.float32),
            pltpu.SemaphoreType.DMA((3,)),
            pltpu.SemaphoreType.DMA,
            pltpu.SemaphoreType.DMA((ARRIVALS,)),
            pltpu.SemaphoreType.DMA,
            pltpu.SemaphoreType.DMA,
            pltpu.SemaphoreType.DMA,
            pltpu.SemaphoreType.DMA,
            pltpu.SemaphoreType.REGULAR,
        ],
        compiler_params=pltpu.CompilerParams(
            collective_id=0, has_side_effects=True, vmem_limit_bytes=28 * 1024 * 1024
        ),
    )(fields, mean_old, land_mask)
    mean_new, level_rms = pl.pallas_call(
        write,
        out_shape=(
            jax.ShapeDtypeStruct(mean_old.shape, jnp.float32),
            jax.ShapeDtypeStruct((1, FIELDS), jnp.float32),
        ),
        in_specs=[pl.BlockSpec(memory_space=pltpu.VMEM)] * 2,
        out_specs=[pl.BlockSpec(memory_space=pltpu.HBM)] * 2,
        scratch_shapes=[
            pltpu.VMEM((1, FIELDS), jnp.float32),
            pltpu.SemaphoreType.DMA,
            pltpu.SemaphoreType.DMA,
        ],
        compiler_params=pltpu.CompilerParams(vmem_limit_bytes=8 * 1024 * 1024),
    )(new, sums)
    return mean_new, level_rms.reshape(FIELDS, 1)


def solution(mesh):
    in_specs = (P(None, None, "cmp", "io"), P(None, "cmp", "io", None), P("cmp", "io", None))
    out_specs = (P(None, "cmp", "io", None), P(None, "cmp"))
    return jax.shard_map(
        on_device, mesh=mesh, in_specs=in_specs, out_specs=out_specs, check_vma=False
    )
```

```python
import jax
import jax.numpy as jnp
from jax import lax
from jax.experimental import pallas as pl
from jax.experimental.pallas import tpu as pltpu
from jax.sharding import PartitionSpec as P

STEPS = 3
MESH = pl.DeviceIdType.MESH

FIELDS = 6
LON = 16
ROWS = 64
COLS = 256
CHUNKS = 32
OUT_CHUNKS = 24
GROUPS = ROWS // 8
LAST = FIELDS - 1
MAIN_ROWS, LAST_ROWS = 16, 8
PER_FIELD = ROWS // MAIN_ROWS
LAST_PIECES = MAIN_ROWS // LAST_ROWS
ARRIVALS = LAST + PER_FIELD - 1 + LAST_PIECES
ORDER = [(dx, dy, dc) for dc in (0, 1) for dx in (1, 3, 2, 0) for dy in (0, 1)]


RING_HOPS = (0, 1, 2, 1)
FAR_FIRST = sorted(
    ((dz, dy) for dz in range(4) for dy in range(4) if (dz, dy) != (0, 0)),
    key=lambda d: -RING_HOPS[d[0]] - RING_HOPS[d[1]],
)


def band_at(io, dz, dy):
    return lax.rem(io // 4 + dz, 4) * 4 + lax.rem(lax.rem(io, 4) + dy, 4)


def lanes_of(array, index):
    return jnp.take_along_axis(array, index, axis=1, mode="promise_in_bounds")


def plan_group(g, mask, place, arrive, count):
    rows = pl.ds(pl.multiple_of(g * 8, 8), 8)
    chunk = [mask[rows, pl.ds(c * 128, 128)] for c in range(CHUNKS)]
    stacked = jnp.concatenate(chunk, axis=0).astype(jnp.float32).astype(jnp.bfloat16)
    source = lax.broadcasted_iota(jnp.int32, (128, 256), 0)
    target = lax.broadcasted_iota(jnp.int32, (128, 256), 1)
    upto = ((source <= target) | (target >= 128)).astype(jnp.float32).astype(jnp.bfloat16)
    sums = jnp.dot(stacked, upto, preferred_element_type=jnp.float32).astype(jnp.int32)
    lane = lax.broadcasted_iota(jnp.int32, (8, 128), 1)
    base = jnp.zeros((8, 128), jnp.int32)
    state = []
    for c in range(CHUNKS):
        upto_here = sums[c * 8 : c * 8 + 8, :128]
        number = sums[c * 8 : c * 8 + 8, 128:]
        rank = (lane - base) & 127
        at = jnp.zeros((8, 128), jnp.int32)
        for step in (64, 32, 16, 8, 4, 2, 1):
            seen = lanes_of(upto_here, at + (step - 1))
            at = jnp.where(seen <= rank, at + step, at)
        place[g, pl.ds(c * 8, 8), :] = at
        moved = c - ((base + rank) >> 7)
        state.append(jnp.where(rank < number, moved, 0))
        base = base + number
    count[g] = base
    arrived = [jnp.zeros((8, 128), jnp.int32) for _ in range(CHUNKS)]
    for s in range(5):
        bit = 1 << s
        new_state = []
        for c in range(CHUNKS):
            kept = jnp.where((state[c] & bit) != 0, 0, state[c])
            if c + bit < CHUNKS:
                comes = (state[c + bit] & bit) != 0
                arrived[c] = jnp.where(comes, arrived[c] | bit, arrived[c])
                kept = jnp.where(comes, state[c + bit], kept)
            new_state.append(kept)
        state = new_state
    for c in range(CHUNKS):
        arrive[g, pl.ds(c * 8, 8), :] = arrived[c]


def pack_group(f, g, landed, old, new, place, arrive, count):
    rows = pl.ds(pl.multiple_of(g * 8, 8), 8)
    value = []
    for c in range(CHUNKS):
        raw = landed[f, c // 2, rows, pl.ds((c % 2) * 128, 128)]
        value.append(lanes_of(raw, place[g, pl.ds(c * 8, 8), :]))
    moves = [arrive[g, pl.ds(c * 8, 8), :] for c in range(CHUNKS)]
    for s in range(5):
        bit = 1 << s
        for c in range(CHUNKS - bit):
            if s < 4 or c < OUT_CHUNKS:
                value[c] = jnp.where((moves[c] & bit) != 0, value[c + bit], value[c])
    lane = lax.broadcasted_iota(jnp.int32, (8, 128), 1)
    left = count[g] - lane
    squares = jnp.zeros((8, 128), jnp.float32)
    for c in range(OUT_CHUNKS):
        columns = pl.ds(c * 128, 128)
        mean = (STEPS * old[f, rows, columns] + value[c]) * jnp.float32(1.0 / (STEPS + 1.0))
        mean = jnp.where(left > c * 128, mean, jnp.float32(0.0))
        new[f, 0, rows, columns] = mean
        squares = squares + mean * mean
    return squares


def kernel(
    fields, mean_old, land_mask, new, sums,
    staged, landed, mask, old, place, arrive, count, total, parts,
    stage_sem, send_sem, recv_sem, mask_sem, old_sem, part_send, part_recv, group_sem,
):
    io, b = lax.axis_index("io"), lax.axis_index("cmp")
    x, core = b // 2, b % 2
    keeps = (io // 2) == b

    barrier = pltpu.get_barrier_semaphore()
    for dz, dy in FAR_FIRST + [(0, 0)]:
        pl.semaphore_signal(
            barrier, inc=1, device_id=(band_at(io, dz, dy), io // 2), device_id_type=MESH
        )
    def stage(f, first, size, sem):
        return [
            pltpu.make_async_copy(
                fields.at[f, :, pl.ds(half * ROWS + first, size), :],
                staged.at[f, :, pl.ds(half * ROWS + first, size), :],
                stage_sem.at[sem],
            )
            for half in range(2)
        ]

    def staged_wait(f, size, sem):
        both = staged.at[f, :, pl.ds(0, 2 * size), :]
        pltpu.make_async_copy(both, both, stage_sem.at[sem]).wait()

    for copy in stage(0, 0, MAIN_ROWS, 0):
        copy.start()
    mask_copy = pltpu.make_async_copy(land_mask.at[0], mask, mask_sem)
    mask_copy.start()
    for copy in stage(0, MAIN_ROWS, ROWS - MAIN_ROWS, 1):
        copy.start()
    for f in range(1, FIELDS):
        for copy in stage(f, 0, ROWS, 2):
            copy.start()
    old_copy = pltpu.make_async_copy(mean_old.at[:, 0], old, old_sem)
    old_copy.start()

    peers = []
    for dx, dy, dc in ORDER:
        level = lax.rem(x + dx, 4) * 2 + lax.rem(core + dc, 2)
        half = lax.rem((lax.rem(io, 4) + 1) // 2 + 1 + core + dy, 2)
        band = x * 4 + core * 2 + half
        peers.append((level, band, half, (band == io) & (level == b)))

    def send_piece(arrival, f, first, size):
        for level, band, half, here in peers:
            rows = pl.ds(pl.multiple_of(half * ROWS + first, 8), size)
            target = landed.at[f, io, pl.ds(pl.multiple_of(first, 8), size), :]

            @pl.when(jnp.logical_not(here))
            def _():
                pltpu.make_async_remote_copy(
                    src_ref=staged.at[f, level, rows, :],
                    dst_ref=target,
                    send_sem=send_sem,
                    recv_sem=recv_sem.at[arrival],
                    device_id=(band, level),
                    device_id_type=MESH,
                ).start()

            @pl.when(here)
            def _():
                pltpu.make_async_copy(fields.at[f, level, rows, :], target, recv_sem.at[arrival]).start()

    def send_early(i, carry):
        f = i // PER_FIELD
        send_piece(f, f, lax.rem(i, PER_FIELD) * MAIN_ROWS, MAIN_ROWS)
        return carry

    def send_late(i, carry):
        send_piece(LAST + i, LAST, i * MAIN_ROWS, MAIN_ROWS)
        return carry

    staged_wait(0, MAIN_ROWS, 0)
    pl.semaphore_wait(barrier, LON)
    send_early(0, 0)
    staged_wait(0, ROWS - MAIN_ROWS, 1)
    lax.fori_loop(1, PER_FIELD, send_early, 0)
    others = staged.at[pl.ds(1, FIELDS - 1)]
    pltpu.make_async_copy(others, others, stage_sem.at[2]).wait()
    lax.fori_loop(PER_FIELD, LAST * PER_FIELD, send_early, 0)
    lax.fori_loop(0, PER_FIELD - 1, send_late, 0)
    for i in range(LAST_PIECES):
        first = ROWS - MAIN_ROWS + i * LAST_ROWS
        send_piece(LAST + PER_FIELD - 1 + i, LAST, first, LAST_ROWS)

    mask_copy.wait()

    def plan(g, carry):
        plan_group(g, mask, place, arrive, count)
        return carry

    lax.fori_loop(0, GROUPS, plan, 0)
    total[...] = jnp.zeros_like(total)
    old_copy.wait()

    def pack_piece(arrival, f, first, size):
        piece = landed.at[f, :, pl.ds(pl.multiple_of(first, 8), size), :]
        pltpu.make_async_copy(piece, piece, recv_sem.at[arrival]).wait()

        def pack(k, squares):
            return squares + pack_group(f, first // 8 + k, landed, old, new, place, arrive, count)

        total[f] += lax.fori_loop(0, size // 8, pack, jnp.zeros((8, 128), jnp.float32))

    def pack_early(f, carry):
        pack_piece(f, f, 0, ROWS)
        return carry

    def pack_late(i, carry):
        pack_piece(LAST + i, LAST, i * MAIN_ROWS, MAIN_ROWS)
        return carry

    def pack_last(i, carry):
        pack_piece(LAST + PER_FIELD - 1 + i, LAST, ROWS - MAIN_ROWS + i * LAST_ROWS, LAST_ROWS)
        return carry

    pack_early(0, 0)

    @pl.when(io == 2 * b)
    def _():
        for s in range(LON):
            pl.semaphore_signal(group_sem, inc=1, device_id=(s, b), device_id_type=MESH)

    lax.fori_loop(1, LAST, pack_early, 0)
    lax.fori_loop(0, PER_FIELD - 1, pack_late, 0)
    lax.fori_loop(0, LAST_PIECES, pack_last, 0)

    ocean = count[0]
    for g in range(1, GROUPS):
        ocean = ocean + count[g]
    lines = [jnp.sum(total[f], axis=0, keepdims=True) for f in range(FIELDS)]
    lines.append(jnp.sum(ocean.astype(jnp.float32), axis=0, keepdims=True))
    lines.append(jnp.zeros((1, 128), jnp.float32))
    parts[io] = jnp.concatenate(lines, axis=0)

    pl.semaphore_wait(group_sem, 1)
    for dz, dy in FAR_FIRST:
        pltpu.make_async_remote_copy(
            src_ref=parts.at[io],
            dst_ref=parts.at[io],
            send_sem=part_send,
            recv_sem=part_recv,
            device_id=(band_at(io, dz, dy), b),
            device_id_type=MESH,
        ).start()

    @pl.when(jnp.logical_not(keeps))
    def _():
        pltpu.make_async_copy(landed, landed, send_sem).wait()

    @pl.when(keeps)
    def _():
        most = landed.at[:, pl.ds(0, LON - 1)]
        pltpu.make_async_copy(most, most, send_sem).wait()

    others = parts.at[pl.ds(0, LON - 1)]
    pltpu.make_async_copy(others, others, part_send).wait()
    pltpu.make_async_copy(others, others, part_recv).wait()
    everything = parts[0]
    for s in range(1, LON):
        everything = everything + parts[s]
    sums[...] = everything


def write(new, sums, mean_new, level_rms, row, mean_sem, row_sem):
    for f in range(FIELDS):
        pltpu.make_async_copy(new.at[f], mean_new.at[f], mean_sem).start()
    lane = lax.broadcasted_iota(jnp.int32, (1, 128), 1)
    square_sum = jnp.zeros((1, 128), jnp.float32)
    for f in range(FIELDS):
        field_sum = jnp.sum(sums[f : f + 1], axis=1, keepdims=True)
        square_sum = jnp.where(lane == f, field_sum, square_sum)
    ocean_total = sums[FIELDS : FIELDS + 1]
    row[...] = jnp.sqrt(square_sum / ocean_total + 1e-06)[:, :FIELDS]
    row_copy = pltpu.make_async_copy(row, level_rms, row_sem)
    row_copy.start()
    pltpu.make_async_copy(new, mean_new, mean_sem).wait()
    row_copy.wait()


def on_device(fields, mean_old, land_mask):
    fields, mean_old, land_mask = (
        pltpu.with_memory_space_constraint(a, pltpu.HBM) for a in (fields, mean_old, land_mask)
    )
    new, sums = pl.pallas_call(
        kernel,
        out_shape=(
            pltpu.VMEM(mean_old.shape, jnp.float32),
            pltpu.VMEM((8, 128), jnp.float32),
        ),
        in_specs=[pl.BlockSpec(memory_space=pltpu.HBM)] * 3,
        out_specs=[pl.BlockSpec(memory_space=pltpu.VMEM)] * 2,
        scratch_shapes=[
            pltpu.VMEM(fields.shape, jnp.float32),
            pltpu.VMEM((FIELDS, LON, ROWS, COLS), jnp.float32),
            pltpu.VMEM((ROWS, CHUNKS * 128), jnp.int32),
            pltpu.VMEM((FIELDS, ROWS, OUT_CHUNKS * 128), jnp.float32),
            pltpu.VMEM((GROUPS, CHUNKS * 8, 128), jnp.int32),
            pltpu.VMEM((GROUPS, CHUNKS * 8, 128), jnp.int32),
            pltpu.VMEM((GROUPS, 8, 128), jnp.int32),
            pltpu.VMEM((FIELDS, 8, 128), jnp.float32),
            pltpu.VMEM((LON, 8, 128), jnp.float32),
            pltpu.SemaphoreType.DMA((3,)),
            pltpu.SemaphoreType.DMA,
            pltpu.SemaphoreType.DMA((ARRIVALS,)),
            pltpu.SemaphoreType.DMA,
            pltpu.SemaphoreType.DMA,
            pltpu.SemaphoreType.DMA,
            pltpu.SemaphoreType.DMA,
            pltpu.SemaphoreType.REGULAR,
        ],
        compiler_params=pltpu.CompilerParams(
            collective_id=0, has_side_effects=True, vmem_limit_bytes=28 * 1024 * 1024
        ),
    )(fields, mean_old, land_mask)
    mean_new, level_rms = pl.pallas_call(
        write,
        out_shape=(
            jax.ShapeDtypeStruct(mean_old.shape, jnp.float32),
            jax.ShapeDtypeStruct((1, FIELDS), jnp.float32),
        ),
        in_specs=[pl.BlockSpec(memory_space=pltpu.VMEM)] * 2,
        out_specs=[pl.BlockSpec(memory_space=pltpu.HBM)] * 2,
        scratch_shapes=[
            pltpu.VMEM((1, FIELDS), jnp.float32),
            pltpu.SemaphoreType.DMA,
            pltpu.SemaphoreType.DMA,
        ],
        compiler_params=pltpu.CompilerParams(vmem_limit_bytes=8 * 1024 * 1024),
    )(new, sums)
    return mean_new, level_rms.reshape(FIELDS, 1)


def solution(mesh):
    in_specs = (P(None, None, "cmp", "io"), P(None, "cmp", "io", None), P("cmp", "io", None))
    out_specs = (P(None, "cmp", "io", None), P(None, "cmp"))
    return jax.shard_map(
        on_device, mesh=mesh, in_specs=in_specs, out_specs=out_specs, check_vma=False
    )
```
